128 devices in a mesh: rep: 8 (over x_lo, z), fsdp: 16 (over y, x_hi, core).
Axes of the slice: x: 4 (x_hi: 2, x_lo: 2; x = x_hi * 2 + x_lo), y: 4, z: 4, core: 2. Of those that a mesh axis runs over, the one named last changes fastest.
Arguments:
- hidden: bfloat16 [32768, 7168], P(('rep', 'fsdp')), may hold values from -24 to 24
- out_grad: bfloat16 [32768, 2048], P(('rep', 'fsdp')), may hold values from -0.09375 to 0.09375
- inner_params: float32 [8, 7168, 2048], P('rep', 'fsdp'), may hold values from -0.132 to 0.132
- first_moment: bfloat16 [8, 7168, 2048], P('rep', 'fsdp'), may hold values from -6 to 6
- second_moment: bfloat16 [8, 7168, 2048], P('rep', 'fsdp'), may hold values from 0.049804688 to 2
- outer_params: float32 [7168, 2048], P('fsdp', 'rep'), may hold values from -0.12 to 0.12
- outer_momentum: float32 [7168, 2048], P('fsdp', 'rep'), may hold values from -0.012 to 0.012
Outputs:
- new_params: float32 [7168, 2048], P('fsdp')
- new_momentum: float32 [7168, 2048], P('fsdp', 'rep')
- new_first: bfloat16 [8, 7168, 2048], P('rep', 'fsdp')
- new_second: bfloat16 [8, 7168, 2048], P('rep', 'fsdp')
The draws below stay inside these ranges and needn't reach their ends.
All inputs are finite; a program needn't handle non-finite values.
Results may differ from the reference program's by a relative error of at most 0.009.
Values may be sent and summed in bfloat16 or wider, within the bound.
A program may use at most 192 MiB of HBM per device.

```python
import math
import jax
import jax.numpy as jnp
from jax import lax

FFW = 7168
DW = 2048
TOK_DEV = 256
INNER_STEP = 500
REPLICAS = 8
TOKENS = 32768
N_FSDP = 16


def base_weights(key):
    inner_key = jax.random.fold_in(key, 11)
    values = jax.random.normal(inner_key, (FFW, DW), jnp.float32)
    return jnp.clip(0.02 * values, -0.12, 0.12)


def draw_outer_params(key, part):
    return base_weights(key)


def draw_inner_params(key, part):
    drift_key = jax.random.fold_in(key, 13)
    drift = jax.random.normal(drift_key, (REPLICAS, FFW, DW), jnp.float32)
    drift = jnp.clip(0.002 * drift, -0.012, 0.012)
    return base_weights(key)[None] + drift


def with_spikes(array, stream_key, source, target, shards_of, factor):
    owner, partner = [(jnp.arange(array.shape[dim]) // (array.shape[dim] // shards_of)).reshape([-1 if axis == dim else 1 for axis in range(array.ndim)]) for dim in (source, target)]
    chosen = jax.random.permutation(stream_key, shards_of)[partner]
    strong = (owner == chosen) | (owner == (partner + shards_of // 2) % shards_of)
    return jnp.where(strong, factor * array, array)


def level_of(stream_key, extent, shards, smallest, top_value):
    def one(position, shards_of):
        draws = jax.random.uniform(jax.random.fold_in(jax.random.fold_in(stream_key, 6), position), (shards_of,), jnp.float32, smallest / len(shards), top_value / len(shards))
        return jnp.repeat(jnp.exp(draws), extent[position] // shards_of).reshape((-1,) + (1,) * (len(extent) - position - 1))

    level = one(*shards[0])
    for cut in shards[1:]:
        level = level * one(*cut)
    return level


def noise(own_key, shape, spread, most, cuts=(), kind=jnp.bfloat16):
    values = spread * jax.random.normal(own_key, shape, jnp.float32)
    if cuts:
        values = values * level_of(own_key, shape, cuts, -0.22, 0.18)
    return jnp.clip(values, -most, most).astype(kind)


def bell_draw_with(key, dims, deviation, most, pieces, heavy, held_as=jnp.bfloat16):
    result = deviation * jax.random.normal(key, dims, jnp.float32)
    if pieces:
        result = result * level_of(key, dims, pieces, -0.22, 0.18)
    return jnp.clip(with_spikes(result, jax.random.fold_in(key, 3), *heavy), -most, most).astype(held_as)


def setup_inputs(seed: int = 0) -> dict:
    streams_of = jax.random.split(jax.random.key(seed), 8)
    return {
        "hidden": bell_draw_with(streams_of[0], (TOKENS, FFW), 1.0, 24.0, ((0, 128),), (0, 1, 128, 5.5)),
        "out_grad": noise(streams_of[1], (TOKENS, DW), (TOK_DEV * N_FSDP) ** -0.5, 0.09375, ((0, 128),)),
        "inner_params": draw_inner_params(jax.random.fold_in(streams_of[7], 71), 0),
        "first_moment": noise(streams_of[3], (REPLICAS, FFW, DW), 1.0, 6.0, ((0, 8), (1, 16))),
        "second_moment": jnp.clip(jnp.exp(math.log(2.0) - 3.6927934 * jax.random.uniform(streams_of[4], (REPLICAS, FFW, DW), jnp.float32) ** level_of(streams_of[4], (REPLICAS, FFW, DW), ((0, 8), (1, 16)), -0.2, 0.2)), 0.049804688, 2.0).astype(jnp.bfloat16),
        "outer_params": draw_outer_params(jax.random.fold_in(streams_of[7], 71), 0),
        "outer_momentum": noise(streams_of[6], (FFW, DW), 0.002, 0.012, ((0, 16), (1, 8)), jnp.float32),
    }


beta_one = 0.9
beta_two = 0.95
epsilon = 1e-08
inner_rate = 0.0004
weight_decay = 0.1
outer_rate = 0.7
nesterov = 0.9

def add_block(running, block_pair):
    hidden_block, grad_block = block_pair
    partial_value = jnp.dot(hidden_block.T, grad_block, preferred_element_type=jnp.float32)
    rounded = lax.optimization_barrier(partial_value.astype(jnp.bfloat16)).astype(jnp.float32)
    return (running + rounded, None)

def replica_step(running, inputs):
    hidden_blocks, grad_blocks, params, first_state, second = inputs
    gradient, unused = lax.scan(add_block, jnp.zeros((FFW, DW), jnp.float32), (hidden_blocks, grad_blocks))
    moment_one = beta_one * first_state.astype(jnp.float32) + (1.0 - beta_one) * gradient
    moment_two = beta_two * second.astype(jnp.float32) + (1.0 - beta_two) * gradient * gradient
    corrected_one = moment_one / (1.0 - beta_one ** INNER_STEP)
    corrected_two = moment_two / (1.0 - beta_two ** INNER_STEP)
    stepped = params - inner_rate * (corrected_one / (jnp.sqrt(corrected_two) + epsilon) + weight_decay * params)
    return (running + stepped, (moment_one.astype(jnp.bfloat16), moment_two.astype(jnp.bfloat16)))

def reference(hidden, out_grad, inner_params, first_moment, second_moment, outer_params, outer_momentum):
    hidden_blocks = hidden.reshape(REPLICAS, N_FSDP, TOK_DEV, FFW)
    grad_blocks = out_grad.reshape(REPLICAS, N_FSDP, TOK_DEV, DW)
    summed, moments = lax.scan(replica_step, jnp.zeros((FFW, DW), jnp.float32), (hidden_blocks, grad_blocks, inner_params, first_moment, second_moment))
    outer_delta = outer_params - summed / REPLICAS
    new_momentum = nesterov * outer_momentum + outer_delta
    new_params = outer_params - outer_rate * (outer_delta + nesterov * new_momentum)
    return (new_params, new_momentum, moments[0], moments[1])
```

```python
import functools

import jax
import jax.numpy as jnp
from jax import lax
from jax.experimental import pallas as pl
from jax.experimental.pallas import tpu as pltpu
from jax.sharding import PartitionSpec as P

INNER_STEP = 500

beta_one = 0.9
beta_two = 0.95
epsilon = 1e-08
inner_rate = 0.0004
weight_decay = 0.1
outer_rate = 0.7
nesterov = 0.9

MESH = pl.DeviceIdType.MESH
BF16, F32 = jnp.bfloat16, jnp.float32

CUTS = (112, 112)
OFFS = tuple(sum(CUTS[:p]) for p in range(len(CUTS)))
ORDER = ((0, 0), (1, 0), (0, 1), (1, 1), (0, 2), (1, 2), (0, 3), (1, 3))
PIPES = len(CUTS)
ROWS, COLS, TOK, REP, YS = 448, 2048, 256, 8, 4
HALF = ROWS // 2
OWN = COLS // REP
PEERS = tuple((dx, dz) for dx in range(2) for dz in range(4) if (dx, dz) != (0, 0))


def rem(a, b):
    return lax.rem(a, jnp.int32(b))


def div(a, b):
    return lax.div(a, jnp.int32(b))


def kernel(
    hid, og, ip, fm, sm, op, om,
    o_np, o_nm, o_nf, o_ns,
    hv, hs, hg, ogg, ysend, yrecv, ipv, fmv, smv, opv, omv, stp, rsb, agb,
    ld, ldh, stq, ogs, ogr, hss, hsr, yss, ysr, rss, rsr, ags, agr,
):
    r, f = lax.axis_index("rep"), lax.axis_index("fsdp")
    xl, z = div(r, 4), rem(r, 4)
    y, xh, c = div(f, 4), rem(div(f, 2), 2), rem(f, 2)

    def at(yy, xx, cc):
        return (r, yy * 4 + xx * 2 + cc)

    mate, opp, opp_mate = at(y, xh, 1 - c), at(y, 1 - xh, c), at(y, 1 - xh, 1 - c)
    targets = (mate, opp, opp_mate)
    up, down = at(rem(y + 1, 4), xh, c), at(rem(y + 3, 4), xh, c)

    def peer_rep(dx, dz):
        return rem(xl + dx, 2) * 4 + rem(z + dz, 4)

    def slot(dx, dz):
        return PEERS.index((dx, dz % 4))

    def chunk_cols(s, xx):
        yy = rem(y + 3 - s + 4, 4)
        return pl.multiple_of((yy * 2 + xx) * 896, 128)

    def send(src, dst, ss, rs, to):
        return pltpu.make_async_remote_copy(
            src_ref=src, dst_ref=dst, send_sem=ss, recv_sem=rs, device_id=to, device_id_type=MESH
        )

    og_in = pltpu.make_async_copy(og, ogg.at[pl.ds(0, TOK)], ld.at[0])
    og_in.start()
    chunk_order = tuple((s, o) for o in (1, 0) for s in (0, 2, 1, 3))
    loads = {}
    for i, (s, o) in enumerate(chunk_order):
        xx = rem(xh + o, 2)
        loads[s, o] = pltpu.make_async_copy(
            hid.at[:, pl.ds(chunk_cols(s, xx), 896)], hv.at[i], ldh.at[i]
        )
        loads[s, o].start()
    state_in = [
        pltpu.make_async_copy(a, b, ld.at[1 + i])
        for i, (a, b) in enumerate(((fm.at[0], fmv), (sm.at[0], smv), (ip.at[0], ipv), (op, opv), (om, omv)))
    ]
    for q in state_in:
        q.start()

    barrier = pltpu.get_barrier_semaphore()
    friends = list(targets) + [up, down] + [(peer_rep(dx, dz), f) for dx, dz in PEERS]
    for d in friends:
        pl.semaphore_signal(barrier, inc=1, device_id=d, device_id_type=MESH)
    pl.semaphore_wait(barrier, len(friends))

    og_in.wait()
    own_og = ogg.at[pl.ds(0, TOK)]
    og_x = send(own_og, ogg.at[pl.ds(2 * TOK, TOK)], ogs.at[1], ogr.at[1], opp)
    og_d = send(own_og, ogg.at[pl.ds(TOK, TOK)], ogs.at[0], ogr.at[0], mate)
    og_f = send(
        ogg.at[pl.ds(2 * TOK, TOK)], ogg.at[pl.ds(3 * TOK, TOK)], ogs.at[2], ogr.at[2], mate
    )
    og_x.start()
    og_d.start()

    for i, (s, o) in enumerate(chunk_order):
        loads[s, o].wait()
        turned = hv[i].T
        s_down = (2 - s) % 4
        for p in range(PIPES):
            m, off = CUTS[p], OFFS[p]
            for cc in range(2):
                top = turned[448 * cc + off : 448 * cc + off + m]
                low = turned[448 * cc + HALF + off : 448 * cc + HALF + off + m]
                same = c == cc

                def put(t_same, t_other):
                    for t, cond in ((t_same, same), (t_other, jnp.logical_not(same))):

                        @pl.when(cond)
                        def _(t=t):
                            if t is None:
                                hg[s, 2 * off : 2 * off + m, 0:TOK] = top
                                hg[s_down, 2 * off + m : 2 * off + 2 * m, 0:TOK] = low
                            else:
                                hs[t, s, 2 * off : 2 * off + m, :] = top
                                hs[t, s_down, 2 * off + m : 2 * off + 2 * m, :] = low

                if o:
                    put(1, 2)
                else:
                    put(None, 0)

    hid_copies = {}
    for p, s in ORDER:
        rows = pl.ds(2 * OFFS[p], 2 * CUTS[p])
        for t in (1, 2, 0):
            q = send(
                hs.at[t, s, rows],
                hg.at[s, rows, pl.ds(TOK * (t + 1), TOK)],
                hss.at[p, s, t], hsr.at[p, s, t], targets[t],
            )
            q.start()
            hid_copies[p, s, t] = q

    og_d.wait_recv()
    og_x.wait_recv()
    og_f.start()
    og_f.wait_recv()

    y_copies, rs_copies, ag_copies = {}, {}, {}
    loaded = False

    def partial(p, s, n):
        rows = slice(2 * OFFS[p], 2 * OFFS[p] + 2 * CUTS[p])
        cols = pl.ds(pl.multiple_of(n * OWN, OWN), OWN)
        got = jnp.dot(hg[s, rows, :], ogg[:, cols], preferred_element_type=F32)
        if s:
            got = got + yrecv[s - 1, rows, cols].astype(F32)
        return got

    for p, s in ORDER:
        m, off = CUTS[p], OFFS[p]
        rows = slice(2 * off, 2 * off + 2 * m)
        for t in range(3):
            hid_copies[p, s, t].wait_recv()
        if s:
            for q in y_copies[p, s - 1]:
                q.wait_recv()
        if s < 3:

            @pl.loop(0, REP)
            def _(n):
                cols = pl.ds(pl.multiple_of(n * OWN, OWN), OWN)
                ysend[s, rows, cols] = partial(p, s, n).astype(BF16)

            y_copies[p, s] = [
                send(
                    ysend.at[s, pl.ds(start, m)], yrecv.at[s, pl.ds(start, m)],
                    yss.at[p, s, i], ysr.at[p, s, i], to,
                )
                for i, (start, to) in enumerate(((2 * off, up), (2 * off + m, down)))
            ]
            for q in y_copies[p, s]:
                q.start()
            continue
        if not loaded:
            for q in state_in:
                q.wait()
            loaded = True

        @pl.loop(0, REP)
        def _(n):
            cols = pl.ds(pl.multiple_of(n * OWN, OWN), OWN)
            gradient = partial(p, s, n)
            for i, start in enumerate((off, HALF + off)):
                g = gradient[i * m : (i + 1) * m]
                at_rows = slice(start, start + m)
                one = beta_one * fmv[at_rows, cols].astype(F32) + (1.0 - beta_one) * g
                two = beta_two * smv[at_rows, cols].astype(F32) + (1.0 - beta_two) * g * g
                fmv[at_rows, cols] = one.astype(BF16)
                smv[at_rows, cols] = two.astype(BF16)
                w = ipv[at_rows, cols]
                hat_one = one * (1.0 / (1.0 - beta_one**INNER_STEP))
                hat_two = two * (1.0 / (1.0 - beta_two**INNER_STEP))
                stp[n, 2 * off + i * m : 2 * off + (i + 1) * m, :] = w - inner_rate * (
                    hat_one / (jnp.sqrt(hat_two) + epsilon) + weight_decay * w
                )

        span = pl.ds(2 * off, 2 * m)
        rs_copies[p] = []
        for dx, dz in PEERS:
            there, k = peer_rep(dx, dz), slot(dx, -dz)
            q = send(stp.at[there, span], rsb.at[k, span], rss.at[p, k], rsr.at[p, k], (there, f))
            q.start()
            rs_copies[p].append(q)

    stores = []
    for j, (a, b) in enumerate(((fmv, o_nf), (smv, o_ns))):
        q = pltpu.make_async_copy(a, b, stq.at[j])
        q.start()
        stores.append(q)

    for p in range(PIPES):
        m, off = CUTS[p], OFFS[p]
        span = pl.ds(2 * off, 2 * m)
        for q in rs_copies[p]:
            q.wait_recv()
        rows = slice(2 * off, 2 * off + 2 * m)
        summed = stp[r, rows, :]
        for k in range(len(PEERS)):
            summed = summed + rsb[k, rows, :]
        for i, start in enumerate((off, HALF + off)):
            at_rows = slice(start, start + m)
            params = opv[at_rows, :]
            delta = params - summed[i * m : (i + 1) * m] / REP
            momentum = nesterov * omv[at_rows, :] + delta
            omv[at_rows, :] = momentum
            agb[r, 2 * off + i * m : 2 * off + (i + 1) * m, :] = (
                params - outer_rate * (delta + nesterov * momentum)
            ).astype(BF16)
        ag_copies[p] = []
        for dx, dz in PEERS:
            there, k = peer_rep(dx, dz), slot(dx, -dz)
            q = send(agb.at[r, span], agb.at[r, span], ags.at[p, k], agr.at[p, k], (there, f))
            q.start()
            ag_copies[p].append(q)

    q = pltpu.make_async_copy(omv, o_nm, stq.at[2])
    q.start()
    stores.append(q)
    for p in range(PIPES):
        m, off = CUTS[p], OFFS[p]
        span = pl.ds(2 * off, 2 * m)
        for q in ag_copies[p]:
            q.wait_recv()
        for k in range(REP):
            for i, start in enumerate((off, HALF + off)):
                q = pltpu.make_async_copy(
                    agb.at[k, pl.ds(2 * off + i * m, m)],
                    o_np.at[pl.ds(start, m), pl.ds(k * OWN, OWN)],
                    stq.at[3 + (p * REP + k) * 2 + i],
                )
                q.start()
                stores.append(q)

    for q in (og_x, og_d, og_f):
        q.wait_send()
    for q in hid_copies.values():
        q.wait_send()
    for group in (y_copies, rs_copies, ag_copies):
        for qs in group.values():
            for q in qs:
                q.wait_send()
    for q in stores:
        q.wait()


def per_device(hidden, out_grad, inner_params, first, second, outer_params, outer_momentum):
    any_ = pl.BlockSpec(memory_space=pl.ANY)
    dma = pltpu.SemaphoreType.DMA
    n = len(PEERS)
    params, momentum, one, two = pl.pallas_call(
        kernel,
        out_shape=(
            jax.ShapeDtypeStruct((ROWS, COLS), BF16),
            jax.ShapeDtypeStruct((ROWS, OWN), F32),
            jax.ShapeDtypeStruct((ROWS, COLS), BF16),
            jax.ShapeDtypeStruct((ROWS, COLS), BF16),
        ),
        in_specs=[any_] * 7,
        out_specs=(any_,) * 4,
        scratch_shapes=[
            pltpu.VMEM((8, TOK, 896), BF16),
            pltpu.VMEM((3, YS, ROWS, TOK), BF16),
            pltpu.VMEM((YS, ROWS, 4 * TOK), BF16),
            pltpu.VMEM((4 * TOK, COLS), BF16),
            pltpu.VMEM((3, ROWS, COLS), BF16),
            pltpu.VMEM((3, ROWS, COLS), BF16),
            pltpu.VMEM((ROWS, COLS), F32),
            pltpu.VMEM((ROWS, COLS), BF16),
            pltpu.VMEM((ROWS, COLS), BF16),
            pltpu.VMEM((ROWS, OWN), F32),
            pltpu.VMEM((ROWS, OWN), F32),
            pltpu.VMEM((REP, ROWS, OWN), F32),
            pltpu.VMEM((n, ROWS, OWN), F32),
            pltpu.VMEM((REP, ROWS, OWN), BF16),
            dma((6,)),
            dma((8,)),
            dma((3 + PIPES * REP * 2,)),
            dma((3,)),
            dma((3,)),
            dma((PIPES, YS, 3)),
            dma((PIPES, YS, 3)),
            dma((PIPES, 3, 2)),
            dma((PIPES, 3, 2)),
            dma((PIPES, n)),
            dma((PIPES, n)),
            dma((PIPES, n)),
            dma((PIPES, n)),
        ],
        compiler_params=pltpu.CompilerParams(
            collective_id=1, has_side_effects=True, vmem_limit_bytes=60_000_000
        ),
        name="step",
    )(hidden, out_grad, inner_params, first, second, outer_params, outer_momentum)
    return params.astype(F32), momentum, one[None], two[None]


def solution(mesh):
    return jax.shard_map(
        per_device,
        mesh=mesh,
        in_specs=(
            P(("rep", "fsdp"), None),
            P(("rep", "fsdp"), None),
            P("rep", "fsdp", None),
            P("rep", "fsdp", None),
            P("rep", "fsdp", None),
            P("fsdp", "rep"),
            P("fsdp", "rep"),
        ),
        out_specs=(
            P("fsdp", None),
            P("fsdp", "rep"),
            P("rep", "fsdp", None),
            P("rep", "fsdp", None),
        ),
        check_vma=False,
    )
```

```python
import functools

import jax
import jax.numpy as jnp
from jax import lax
from jax.experimental import pallas as pl
from jax.experimental.pallas import tpu as pltpu
from jax.sharding import PartitionSpec as P

INNER_STEP = 500

beta_one = 0.9
beta_two = 0.95
epsilon = 1e-08
inner_rate = 0.0004
weight_decay = 0.1
outer_rate = 0.7
nesterov = 0.9

MESH = pl.DeviceIdType.MESH
BF16, F32 = jnp.bfloat16, jnp.float32

CUTS = (64, 64, 16, 32, 16, 32)
OUT = 5
OFFS = tuple(sum(CUTS[:p]) for p in range(len(CUTS)))
PIPES = len(CUTS)
ROWS, COLS, TOK, REP, YS = 448, 2048, 256, 8, 4
HALF = ROWS // 2
OWN = COLS // REP
PARTS = 4
WIDE = COLS // PARTS
LEAVE = (
    (-1, 0), (0, 0), (1, 0), (2, 0), (-1, 1), (-1, 2), (-1, 3), (3, 0), (4, 0), (0, 1), (1, 1), (2, 1), (3, 1),
    (4, 1), (0, 2), (1, 2), (2, 2), (3, 2), (4, 2), (0, 3), (1, 3), (2, 3), (3, 3), (4, 3),
)
TASKS = (
    ("out", 0), ("fwd", 0), ("unit", 0, 0, 0), ("out", 1), ("unit", 2, 0, 0), ("fwd", 1), ("unit", 1, 0, 0),
    ("out", 2), ("unit", 1, 0, 1), ("fwd", 2), ("unit", 1, 0, 2), ("unit", 0, 0, 2), ("unit", 0, 0, 1),
    ("unit", 2, 0, 2), ("fwd", 3), ("out", 3), ("unit", 2, 0, 1), ("unit", 2, 0, 3), ("unit", 0, 0, 3),
    ("unit", 1, 0, 3), ("unit", 3, 0), ("unit", 0, 1), ("unit", 4, 0), ("unit", 1, 1), ("unit", 0, 2),
    ("unit", 3, 1), ("unit", 1, 2), ("adam", 0), ("unit", 4, 1), ("unit", 2, 1), ("inner",), ("adam", 5),
    ("unit", 3, 2), ("adam", 1), ("unit", 4, 2), ("rz", 0), ("unit", 2, 2), ("adam", 3), ("rz", 5), ("adam", 4),
    ("adam", 2), ("rz", 1), ("outer", 0), ("rz", 3), ("rz", 4), ("outer", 5), ("rz", 2), ("outer", 1), ("outer", 3),
    ("outer", 2), ("pass", 5), ("outer", 4), ("pass", 0), ("pass", 1), ("pass", 2), ("pass", 3), ("pass", 4),
    ("end", 1), ("end", 4), ("end", 3), ("end", 5), ("end", 0), ("end", 2),
)
GATHER = "zxxzzx"


def rem(a, b):
    return lax.rem(a, jnp.int32(b))


def div(a, b):
    return lax.div(a, jnp.int32(b))


def kernel(
    hid, og, ip, fm, sm, op, om,
    o_np, o_nm, o_nf, o_ns,
    hv, hs, hg, ogg, acc, ysend, yrecv, ipv, fmv, smv, opv, omv, stp, rsz, xsend, xkeep, xrecv, agb,
    ipr, ips, ipk, hse, hge, ace, yse, yre, xse, xre,
    ld, ldh, stq, ogs, ogm, ogx, ogr, hes, her, yes, yer, xes, xer,
    hss, hsr, yss, ysr, ysp, rzs, rzr, rxs, rxr, axs, axr, azs, azr,
    ips_, ipr_,
):
    scope = jax.named_scope
    r, f = lax.axis_index("rep"), lax.axis_index("fsdp")
    xl, z = div(r, 4), rem(r, 4)
    y, xh, c = div(f, 4), rem(div(f, 2), 2), rem(f, 2)

    def at(yy, xx, cc):
        return (r, yy * 4 + xx * 2 + cc)

    mate, opp, opp_mate = at(y, xh, 1 - c), at(y, 1 - xh, c), at(y, 1 - xh, 1 - c)
    targets = (mate, opp, opp_mate)
    up, down = at(rem(y + 1, 4), xh, c), at(rem(y + 3, 4), xh, c)
    beside = ((1 - xl) * 4 + z, f)
    column = tuple((xl * 4 + rem(z + d, 4), f) for d in (1, 2, 3))

    def send(src, dst, ss, rs, to):
        q = pltpu.make_async_remote_copy(
            src_ref=src, dst_ref=dst, send_sem=ss, recv_sem=rs, device_id=to, device_id_type=MESH
        )
        return q

    def await_bytes(ref, sem):
        pltpu.make_async_copy(ref, ref, sem).wait()

    og_in = pltpu.make_async_copy(og, ogg.at[pl.ds(0, TOK)], ld.at[0])
    og_in.start()
    chunk_order = tuple((s, o) for o in (1, 0) for s in (0, 2, 1, 3))
    loads = {}
    for i, (s, o) in enumerate(chunk_order):
        yy, xx = rem(y + 3 - s + 4, 4), rem(xh + o, 2)
        first = pl.multiple_of((yy * 2 + xx) * (2 * ROWS), 128)
        loads[s, o] = pltpu.make_async_copy(hid.at[:, pl.ds(first, 2 * ROWS)], hv.at[i], ldh.at[i])
        loads[s, o].start()
    state_in = [
        pltpu.make_async_copy(a, b, ld.at[1 + i])
        for i, (a, b) in enumerate(((fm.at[0], fmv), (sm.at[0], smv), (ip.at[0], ipv), (op, opv), (om, omv)))
    ]
    for q in state_in:
        q.start()

    barrier = pltpu.get_barrier_semaphore()
    across = tuple(((1 - xl) * 4 + rem(z + d, 4), f) for d in (1, 2, 3))
    friends = [*targets, up, down, beside, *column] + ([*across] if "d" in GATHER else [])
    for d in friends:
        pl.semaphore_signal(barrier, inc=1, device_id=d, device_id_type=MESH)
    with scope("greet"):
        pl.semaphore_wait(barrier, len(friends))
    with scope("og_in"):
        og_in.wait()

    def part_of(source, k):
        return ogg.at[pl.ds(source * TOK, TOK), pl.ds(k * WIDE, WIDE)]

    og_mate = [send(part_of(0, k), part_of(1, k), ogs, ogm, mate) for k in range(PARTS)]
    og_opp = [send(part_of(0, k), part_of(2, k), ogs, ogx.at[k], opp) for k in range(PARTS)]
    og_pass = [send(part_of(2, k), part_of(3, k), ogs, ogr.at[k], mate) for k in range(PARTS)]
    og_opp[0].start()
    for q in og_mate:
        q.start()

    for i, (s, o) in enumerate(chunk_order):
        with scope(f"turn{i}"):
            loads[s, o].wait()
            turned = hv[i].T
            s_down = (2 - s) % 4
            for cc in range(2):
                for p in range(PIPES):
                    m, off = CUTS[p], OFFS[p]
                    top = turned[ROWS * cc + off : ROWS * cc + off + m]
                    low = turned[ROWS * cc + HALF + off : ROWS * cc + HALF + off + m]
                    if p == OUT:

                        @pl.when(c == cc)
                        def _():
                            hge[s, o * m : (o + 1) * m, 0:TOK] = top
                            hge[s_down, (2 + o) * m : (3 + o) * m, 0:TOK] = low

                        @pl.when(c != cc)
                        def _():
                            hse[s, o * m : (o + 1) * m, :] = top
                            hse[s_down, (2 + o) * m : (3 + o) * m, :] = low

                        continue
                    for t, cond in (((1, c == cc), (2, c != cc)) if o else ((None, c == cc), (0, c != cc))):

                        @pl.when(cond)
                        def _(t=t):
                            if t is None:
                                hg[s, 2 * off : 2 * off + m, 0:TOK] = top
                                hg[s_down, 2 * off + m : 2 * off + 2 * m, 0:TOK] = low
                            else:
                                hs[t, s, 2 * off : 2 * off + m, :] = top
                                hs[t, s_down, 2 * off + m : 2 * off + 2 * m, :] = low

    for s in range(YS):
        send(hse.at[s], hge.at[s, :, pl.ds(TOK, TOK)], hes, her.at[s], mate).start()
    for p, s in LEAVE:
        if p < 0:
            if s:
                og_opp[s].start()
            continue
        rows = pl.ds(2 * OFFS[p], 2 * CUTS[p])
        for t in (1, 2, 0):
            q = send(
                hs.at[t, s, rows],
                hg.at[s, rows, pl.ds(TOK * (t + 1), TOK)],
                hss, hsr.at[p, s], targets[t],
            )
            q.start()

    state_in[2].wait()
    for d in (1, 2, 3):
        there = rem(z + d, 4)
        for side in range(2):
            cols = pl.ds(pl.multiple_of((side * 4 + there) * OWN, OWN), OWN)
            q = send(ipv.at[:, cols], ipr.at[3 - d, side], ips_, ipr_, column[d - 1])
            q.start()

    def sum_inner():
        once("ip", ipr, ipr_)
        with scope("sum_ip"):
            for ref, side in ((ips, 1 - xl), (ipk, xl)):
                cols = pl.ds(pl.multiple_of((side * 4 + z) * OWN, OWN), OWN)
                ref[...] = (ipv[:, cols] + ipr[0, side]) + (ipr[1, side] + ipr[2, side])

    done = set()

    def once(key, ref, sem):
        if key in done:
            return
        done.add(key)
        with scope("w_" + key):
            await_bytes(ref, sem)

    def product(p, s, n, width):
        rows = slice(2 * OFFS[p], 2 * OFFS[p] + 2 * CUTS[p])
        cols = pl.ds(pl.multiple_of(n * width, width), width)
        return rows, cols, jnp.dot(hg[s, rows, :], ogg[:, cols], preferred_element_type=F32)

    def rows_of(p):
        return pl.ds(2 * OFFS[p], 2 * CUTS[p])

    in_parts = set()

    def y_wait(p, s):
        if s == 0 and p in in_parts:
            for k in range(PARTS):
                once(f"y{p}{s}{k}", yrecv.at[s, rows_of(p), pl.ds(k * WIDE, WIDE)], ysp.at[p, k])
        else:
            once(f"y{p}{s}", yrecv.at[s, rows_of(p)], ysr.at[p, s])

    def unit(p, s, part=None):
        m, off = CUTS[p], OFFS[p]
        parts = range(PARTS) if part is None else (part,)
        once(f"hid{p}{s}", hg.at[s, rows_of(p), pl.ds(TOK, 3 * TOK)], hsr.at[p, s])
        for k in parts:
            once(f"og{k}", part_of(3, k), ogr.at[k])
        with scope(f"mm{p}{s}"):

            @pl.loop(parts[0], parts[-1] + 1)
            def _(n):
                rows, cols, got = product(p, s, n, WIDE)
                if s:
                    acc[rows, cols] = got
                else:
                    ysend[s, rows, cols] = got.astype(BF16)

        if s:
            y_wait(p, s - 1)
        if s == 3:
            return
        if s:
            with scope(f"add{p}{s}"):

                @pl.loop(0, REP)
                def _(n):
                    rows, cols = slice(2 * off, 2 * off + 2 * m), pl.ds(pl.multiple_of(n * OWN, OWN), OWN)
                    ysend[s, rows, cols] = (acc[rows, cols] + yrecv[s - 1, rows, cols].astype(F32)).astype(BF16)

        cols = pl.ds(0, COLS) if part is None else pl.ds(part * WIDE, WIDE)
        for start, to in ((2 * off, up), (2 * off + m, down)):
            there = (s, pl.ds(start, m), cols)
            arrived = ysr.at[p, s] if part is None else ysp.at[p, part]
            send(ysend.at[there], yrecv.at[there], yss, arrived, to).start()
        if part is not None:
            in_parts.add(p)

    def out_unit(s):
        m, off = CUTS[OUT], OFFS[OUT]
        once("ogm", ogg.at[pl.ds(TOK, TOK)], ogm)
        once(f"hide{s}", hge.at[s, :, pl.ds(TOK, TOK)], her.at[s])
        with scope(f"mme{s}"):

            @pl.loop(0, PARTS)
            def _(n):
                cols = pl.ds(pl.multiple_of(n * WIDE, WIDE), WIDE)
                got = jnp.dot(hge[s], ogg[0 : 2 * TOK, cols], preferred_element_type=F32)
                if s:
                    ace[:, cols] = got
                else:
                    yse[s, :, cols] = got.astype(BF16)

        if s:
            once(f"ye{s - 1}", yre.at[s - 1], yer.at[s - 1])
            with scope(f"adde{s}"):

                @pl.loop(0, REP)
                def _(n):
                    cols = pl.ds(pl.multiple_of(n * OWN, OWN), OWN)
                    got = ace[:, cols] + yre[s - 1, :, cols].astype(F32)
                    if s < 3:
                        yse[s, :, cols] = got.astype(BF16)
                    else:
                        for i in range(2):
                            acc[2 * off + i * m : 2 * off + (i + 1) * m, cols] = got[2 * i * m : (2 * i + 1) * m]
                            xse[i * m : (i + 1) * m, cols] = got[(2 * i + 1) * m : (2 * i + 2) * m].astype(BF16)

        if s < 3:
            for i, to in enumerate((up, down)):
                there = (s, pl.ds(2 * i * m, 2 * m))
                send(yse.at[there], yre.at[there], yes, yer.at[s], to).start()
        else:
            send(xse, xre, xes, xer, opp).start()

    def adam(p):
        m, off = CUTS[p], OFFS[p]
        if p == OUT:
            once("xe", xre, xer)
        else:
            unit(p, 3)
        if "state" not in done:
            done.add("state")
            for q in (*state_in[:2], *state_in[3:]):
                q.wait()
        with scope(f"adam{p}"):

            @pl.loop(0, REP)
            def _(n):
                cols = pl.ds(pl.multiple_of(n * OWN, OWN), OWN)
                owner_x, owner_z = div(n, 4), rem(n, 4)
                for i, start in enumerate((off, HALF + off)):
                    own_rows, at_rows = slice(2 * off + i * m, 2 * off + (i + 1) * m), slice(start, start + m)
                    last = xre[i * m : (i + 1) * m, cols] if p == OUT else yrecv[2, own_rows, cols]
                    g = acc[own_rows, cols] + last.astype(F32)
                    one = beta_one * fmv[at_rows, cols].astype(F32) + (1.0 - beta_one) * g
                    two = beta_two * smv[at_rows, cols].astype(F32) + (1.0 - beta_two) * g * g
                    fmv[at_rows, cols] = one.astype(BF16)
                    smv[at_rows, cols] = two.astype(BF16)
                    w = ipv[at_rows, cols]
                    hat_one = one * (1.0 / (1.0 - beta_one**INNER_STEP))
                    hat_two = two * (1.0 / (1.0 - beta_two**INNER_STEP))
                    stp[owner_z, owner_x, own_rows, :] = (
                        -inner_rate * (hat_one / (jnp.sqrt(hat_two) + epsilon) + weight_decay * w)
                    ).astype(BF16)

        span = rows_of(p)
        for d in (1, 2, 3):
            there = rem(z + d, 4)
            send(stp.at[there, :, span], rsz.at[3 - d, :, span], rzs, rzr.at[p], column[d - 1]).start()

    def store(a, b, sem):
        pltpu.make_async_copy(a, b, sem).start()

    def reduce_z(p):
        m, off = CUTS[p], OFFS[p]
        rows, span = slice(2 * off, 2 * off + 2 * m), pl.ds(2 * off, 2 * m)
        once(f"rz{p}", rsz.at[:, :, span], rzr.at[p])
        with scope(f"sum{p}"):
            for ref, inner, side in ((xsend, ips, 1 - xl), (xkeep, ipk, xl)):
                a, b, d, e = (
                    v.astype(F32)
                    for v in (stp[z, side, rows, :], rsz[0, side, rows, :], rsz[1, side, rows, :], rsz[2, side, rows, :])
                )
                change = (a + b) + (d + e)
                for i, start in enumerate((off, HALF + off)):
                    ref[2 * off + i * m : 2 * off + (i + 1) * m, :] = (
                        inner[start : start + m, :] + change[i * m : (i + 1) * m]
                    )
        send(xsend.at[span], xrecv.at[span], rxs, rxr.at[p], beside).start()

    def outer(p):
        m, off = CUTS[p], OFFS[p]
        span = pl.ds(2 * off, 2 * m)
        once(f"rx{p}", xrecv.at[span], rxr.at[p])
        with scope(f"outer{p}"):
            for i, start in enumerate((off, HALF + off)):
                own_rows, at_rows = slice(2 * off + i * m, 2 * off + (i + 1) * m), slice(start, start + m)
                params = opv[at_rows, :]
                delta = params - (xkeep[own_rows, :] + xrecv[own_rows, :]) / REP
                momentum = nesterov * omv[at_rows, :] + delta
                omv[at_rows, :] = momentum
                agb[z, xl, own_rows, :] = (params - outer_rate * (delta + nesterov * momentum)).astype(BF16)
        if GATHER[p] == "x":
            give(p, z, xl, axs, axr, beside)
        for to in column:
            give(p, z, xl, azs, azr, to)
        if GATHER[p] != "x":
            give(p, z, xl, axs, axr, beside)
        if GATHER[p] == "d":
            for to in across:
                give(p, z, xl, axs, axr, to)

    def give(p, zz, xx, ss, rs, to):
        here = (zz, xx, rows_of(p))
        send(agb.at[here], agb.at[here], ss, rs.at[p], to).start()

    def pass_on(p):
        if GATHER[p] == "x":
            once(f"ax{p}", agb.at[0, 0, rows_of(p)], axr.at[p])
            for to in column:
                give(p, z, 1 - xl, azs, azr, to)
        else:
            once(f"az{p}", agb.at[pl.ds(0, 3), 0, rows_of(p)], azr.at[p])
            for d in (1, 2, 3):
                give(p, rem(z + d, 4), xl, axs, axr, beside)

    def finish(p):
        m, off = CUTS[p], OFFS[p]
        if GATHER[p] == "x":
            once(f"az{p}", agb.at[pl.ds(0, 3), :, rows_of(p)], azr.at[p])
        else:
            once(f"az{p}", agb.at[pl.ds(0, 3), 0, rows_of(p)], azr.at[p])
            once(f"ax{p}", agb.at[:, 0, rows_of(p)], axr.at[p])
        for zz in range(4):
            for xx in range(2):
                for i, start in enumerate((off, HALF + off)):
                    store(
                        agb.at[zz, xx, pl.ds(2 * off + i * m, m)],
                        o_np.at[pl.ds(start, m), pl.ds((xx * 4 + zz) * OWN, OWN)],
                        stq.at[3],
                    )

    def forward(k):
        once(f"ogx{k}", part_of(2, k), ogx.at[k])
        og_pass[k].start()

    adams, outers = [], []
    run = {
        "out": out_unit, "fwd": forward, "unit": unit, "adam": adam, "rz": reduce_z, "outer": outer,
        "pass": pass_on, "inner": sum_inner, "end": finish,
    }
    for kind, *rest in TASKS:
        run[kind](*rest)
        if kind == "adam":
            adams.append(rest)
            if len(adams) == PIPES:
                store(fmv, o_nf, stq.at[0])
                store(smv, o_ns, stq.at[1])
        if kind == "outer":
            outers.append(rest)
            if len(outers) == PIPES:
                store(omv, o_nm, stq.at[2])

    with scope("drain"):
        await_bytes(ogg.at[pl.ds(0, 3 * TOK)], ogs)
        kept = pl.ds(0, 2 * OFFS[OUT])
        await_bytes(hs.at[:, :, kept], hss)
        await_bytes(ysend.at[:, kept], yss)
        await_bytes(hse, hes)
        await_bytes(yse, yes)
        await_bytes(xse, xes)
        await_bytes(rsz, rzs)
        await_bytes(xsend, rxs)
        for p in range(PIPES):
            x_first = GATHER[p] == "x"
            await_bytes(agb.at[0, 0, rows_of(p)] if x_first else agb.at[:, 0, rows_of(p)], axs)
            await_bytes(agb.at[pl.ds(0, 3), :, rows_of(p)] if x_first else agb.at[pl.ds(0, 3), 0, rows_of(p)], azs)
        await_bytes(ipr, ips_)
        for i, (a, b) in enumerate(((fmv, o_nf), (smv, o_ns), (omv, o_nm))):
            await_bytes(a, stq.at[i])
        await_bytes(fmv, stq.at[3])


def per_device(hidden, out_grad, inner_params, first, second, outer_params, outer_momentum):
    any_ = pl.BlockSpec(memory_space=pl.ANY)
    dma, vmem = pltpu.SemaphoreType.DMA, pltpu.VMEM
    params, momentum, one, two = pl.pallas_call(
        kernel,
        out_shape=(
            jax.ShapeDtypeStruct((ROWS, COLS), BF16),
            jax.ShapeDtypeStruct((ROWS, OWN), F32),
            jax.ShapeDtypeStruct((ROWS, COLS), BF16),
            jax.ShapeDtypeStruct((ROWS, COLS), BF16),
        ),
        in_specs=[any_] * 7,
        out_specs=(any_,) * 4,
        scratch_shapes=[
            vmem((8, TOK, 2 * ROWS), BF16),
            vmem((3, YS, ROWS, TOK), BF16),
            vmem((YS, ROWS, 4 * TOK), BF16),
            vmem((4 * TOK, COLS), BF16),
            vmem((ROWS, COLS), F32),
            vmem((3, ROWS, COLS), BF16),
            vmem((3, ROWS, COLS), BF16),
            vmem((ROWS, COLS), F32),
            vmem((ROWS, COLS), BF16),
            vmem((ROWS, COLS), BF16),
            vmem((ROWS, OWN), F32),
            vmem((ROWS, OWN), F32),
            vmem((4, 2, ROWS, OWN), BF16),
            vmem((3, 2, ROWS, OWN), BF16),
            vmem((ROWS, OWN), F32),
            vmem((ROWS, OWN), F32),
            vmem((ROWS, OWN), F32),
            vmem((4, 2, ROWS, OWN), BF16),
            vmem((3, 2, ROWS, OWN), F32),
            vmem((ROWS, OWN), F32),
            vmem((ROWS, OWN), F32),
            vmem((YS, 4 * CUTS[OUT], TOK), BF16),
            vmem((YS, 4 * CUTS[OUT], 2 * TOK), BF16),
            vmem((4 * CUTS[OUT], COLS), F32),
            vmem((3, 4 * CUTS[OUT], COLS), BF16),
            vmem((3, 4 * CUTS[OUT], COLS), BF16),
            vmem((2 * CUTS[OUT], COLS), BF16),
            vmem((2 * CUTS[OUT], COLS), BF16),
            dma((6,)),
            dma((8,)),
            dma((4,)),
            dma,
            dma,
            dma((PARTS,)),
            dma((PARTS,)),
            dma,
            dma((YS,)),
            dma,
            dma((3,)),
            dma,
            dma,
            dma,
            dma((PIPES, YS)),
            dma,
            dma((PIPES, 3)),
            dma((PIPES, PARTS)),
            dma,
            dma((PIPES,)),
            dma,
            dma((PIPES,)),
            dma,
            dma((PIPES,)),
            dma,
            dma((PIPES,)),
            dma,
            dma,
        ],
        compiler_params=pltpu.CompilerParams(
            collective_id=1, has_side_effects=True, vmem_limit_bytes=60_000_000
        ),
        name="step",
    )(hidden, out_grad, inner_params, first, second, outer_params, outer_momentum)
    return params.astype(F32), momentum, one[None], two[None]


def solution(mesh):
    return jax.shard_map(
        per_device,
        mesh=mesh,
        in_specs=(
            P(("rep", "fsdp"), None),
            P(("rep", "fsdp"), None),
            P("rep", "fsdp", None),
            P("rep", "fsdp", None),
            P("rep", "fsdp", None),
            P("fsdp", "rep"),
            P("fsdp", "rep"),
        ),
        out_specs=(
            P("fsdp", None),
            P("fsdp", "rep"),
            P("rep", "fsdp", None),
            P("rep", "fsdp", None),
        ),
        check_vma=False,
    )
```

```python
import functools

import jax
import jax.numpy as jnp
from jax import lax
from jax.experimental import pallas as pl
from jax.experimental.pallas import tpu as pltpu
from jax.sharding import PartitionSpec as P

INNER_STEP = 500

beta_one = 0.9
beta_two = 0.95
epsilon = 1e-08
inner_rate = 0.0004
weight_decay = 0.1
outer_rate = 0.7
nesterov = 0.9

MESH = pl.DeviceIdType.MESH
BF16, F32 = jnp.bfloat16, jnp.float32

CUTS = (48, 48, 32, 16, 48, 32)
OUT = 5
OFFS = tuple(sum(CUTS[:p]) for p in range(len(CUTS)))
PIPES = len(CUTS)
ROWS, COLS, TOK, REP, YS = 448, 2048, 256, 8, 4
HALF = ROWS // 2
OWN = COLS // REP
PARTS = 4
WIDE = COLS // PARTS
LEAVE = (
    (-1, 0), (2, 0), (1, 0), (-1, 1), (0, 0), (-1, 2), (-1, 3), (2, 1), (4, 0), (3, 0), (0, 1), (3, 1), (1, 1),
    (2, 3), (0, 2), (1, 2), (0, 3), (4, 1), (4, 2), (2, 2), (1, 3), (3, 3), (3, 2), (4, 3),
)
TASKS = (
    ("out", 0), ("fwd", 0), ("unit", 1, 0, 0), ("out", 1), ("fwd", 1), ("unit", 2, 0, 1), ("unit", 1, 0, 1),
    ("out", 2), ("unit", 0, 0, 0), ("fwd", 2), ("unit", 0, 0, 2), ("unit", 2, 0, 0), ("unit", 0, 0, 1),
    ("unit", 1, 0, 2), ("unit", 2, 0, 2), ("fwd", 3), ("unit", 2, 0, 3), ("unit", 1, 0, 3), ("unit", 0, 0, 3),
    ("unit", 4, 0), ("unit", 0, 1), ("unit", 1, 1), ("unit", 0, 2), ("out", 3), ("unit", 1, 2), ("unit", 4, 1),
    ("inner",), ("unit", 2, 1), ("adam", 0), ("adam", 1), ("unit", 4, 2), ("rz", 0), ("unit", 3, 0), ("adam", 5),
    ("unit", 2, 2), ("rz", 1), ("outer", 0), ("adam", 4), ("unit", 3, 1), ("adam", 2), ("rz", 5), ("unit", 3, 2),
    ("outer", 1), ("rz", 4), ("outer", 5), ("adam", 3), ("pass", 0), ("rz", 2), ("outer", 4), ("pass", 1),
    ("rz", 3), ("outer", 2), ("end", 1), ("outer", 3), ("pass", 5), ("end", 0), ("pass", 4), ("end", 2), ("end", 3),
    ("end", 5), ("end", 4),
)
GATHER = "xzddxz"


def rem(a, b):
    return lax.rem(a, jnp.int32(b))


def div(a, b):
    return lax.div(a, jnp.int32(b))


def kernel(
    hid, og, ip, fm, sm, op, om,
    o_np, o_nm, o_nf, o_ns,
    hv, hs, hg, ogg, acc, ysend, yrecv, ipv, fmv, smv, opv, omv, stp, rsz, xsend, xkeep, xrecv, agb,
    ipr, ips, ipk, hse, hge, ace, yse, yre, xse, xre,
    ld, ldh, ogs, ogm, ogx, ogr, hes, her, yes, yer, xes, xer,
    hss, hsr, yss, ysr, ysp, rzs, rzr, rxs, rxr, axs, axr, azs, azr,
    ips_, ipr_,
):
    scope = jax.named_scope
    r, f = lax.axis_index("rep"), lax.axis_index("fsdp")
    xl, z = div(r, 4), rem(r, 4)
    y, xh, c = div(f, 4), rem(div(f, 2), 2), rem(f, 2)

    def at(yy, xx, cc):
        return (r, yy * 4 + xx * 2 + cc)

    mate, opp, opp_mate = at(y, xh, 1 - c), at(y, 1 - xh, c), at(y, 1 - xh, 1 - c)
    targets = (mate, opp, opp_mate)
    up, down = at(rem(y + 1, 4), xh, c), at(rem(y + 3, 4), xh, c)
    beside = ((1 - xl) * 4 + z, f)
    column = tuple((xl * 4 + rem(z + d, 4), f) for d in (1, 2, 3))

    def send(src, dst, ss, rs, to):
        q = pltpu.make_async_remote_copy(
            src_ref=src, dst_ref=dst, send_sem=ss, recv_sem=rs, device_id=to, device_id_type=MESH
        )
        return q

    def await_bytes(ref, sem):
        pltpu.make_async_copy(ref, ref, sem).wait()

    og_in = pltpu.make_async_copy(og, ogg.at[pl.ds(0, TOK)], ld.at[0])
    og_in.start()
    chunk_order = tuple((s, o) for o in (1, 0) for s in (0, 2, 1, 3))
    loads = {}
    for i, (s, o) in enumerate(chunk_order):
        yy, xx = rem(y + 3 - s + 4, 4), rem(xh + o, 2)
        first = pl.multiple_of((yy * 2 + xx) * (2 * ROWS), 128)
        loads[s, o] = pltpu.make_async_copy(hid.at[:, pl.ds(first, 2 * ROWS)], hv.at[i], ldh.at[i])
        loads[s, o].start()
    state_in = [
        pltpu.make_async_copy(a, b, ld.at[1 + i])
        for i, (a, b) in enumerate(((fm.at[0], fmv), (sm.at[0], smv), (ip.at[0], ipv), (op, opv), (om, omv)))
    ]
    for q in state_in:
        q.start()

    barrier = pltpu.get_barrier_semaphore()
    across = tuple(((1 - xl) * 4 + rem(z + d, 4), f) for d in (1, 2, 3))
    friends = [*targets, up, down, beside, *column] + ([*across] if "d" in GATHER else [])
    for d in friends:
        pl.semaphore_signal(barrier, inc=1, device_id=d, device_id_type=MESH)
    with scope("greet"):
        pl.semaphore_wait(barrier, len(friends))
    with scope("og_in"):
        og_in.wait()

    def part_of(source, k):
        return ogg.at[pl.ds(source * TOK, TOK), pl.ds(k * WIDE, WIDE)]

    og_mate = [send(part_of(0, k), part_of(1, k), ogs, ogm, mate) for k in range(PARTS)]
    og_opp = [send(part_of(0, k), part_of(2, k), ogs, ogx.at[k], opp) for k in range(PARTS)]
    og_pass = [send(part_of(2, k), part_of(3, k), ogs, ogr.at[k], mate) for k in range(PARTS)]
    og_opp[0].start()
    for q in og_mate:
        q.start()

    for i, (s, o) in enumerate(chunk_order):
        with scope(f"turn{i}"):
            loads[s, o].wait()
            turned = hv[i].T
            s_down = (2 - s) % 4
            for cc in range(2):
                for p in range(PIPES):
                    m, off = CUTS[p], OFFS[p]
                    top = turned[ROWS * cc + off : ROWS * cc + off + m]
                    low = turned[ROWS * cc + HALF + off : ROWS * cc + HALF + off + m]
                    if p == OUT:

                        @pl.when(c == cc)
                        def _():
                            hge[s, o * m : (o + 1) * m, 0:TOK] = top
                            hge[s_down, (2 + o) * m : (3 + o) * m, 0:TOK] = low

                        @pl.when(c != cc)
                        def _():
                            hse[s, o * m : (o + 1) * m, :] = top
                            hse[s_down, (2 + o) * m : (3 + o) * m, :] = low

                        continue
                    for t, cond in (((1, c == cc), (2, c != cc)) if o else ((None, c == cc), (0, c != cc))):

                        @pl.when(cond)
                        def _(t=t):
                            if t is None:
                                hg[s, 2 * off : 2 * off + m, 0:TOK] = top
                                hg[s_down, 2 * off + m : 2 * off + 2 * m, 0:TOK] = low
                            else:
                                hs[t, s, 2 * off : 2 * off + m, :] = top
                                hs[t, s_down, 2 * off + m : 2 * off + 2 * m, :] = low

    for s in range(YS):
        send(hse.at[s], hge.at[s, :, pl.ds(TOK, TOK)], hes, her.at[s], mate).start()
    for p, s in LEAVE:
        if p < 0:
            if s:
                og_opp[s].start()
            continue
        rows = pl.ds(2 * OFFS[p], 2 * CUTS[p])
        for t in (1, 2, 0):
            q = send(
                hs.at[t, s, rows],
                hg.at[s, rows, pl.ds(TOK * (t + 1), TOK)],
                hss, hsr.at[p, s], targets[t],
            )
            q.start()

    state_in[2].wait()
    for d in (1, 2, 3):
        there = rem(z + d, 4)
        for side in range(2):
            cols = pl.ds(pl.multiple_of((side * 4 + there) * OWN, OWN), OWN)
            q = send(ipv.at[:, cols], ipr.at[3 - d, side], ips_, ipr_, column[d - 1])
            q.start()

    def sum_inner():
        once("ip", ipr, ipr_)
        with scope("sum_ip"):
            for ref, side in ((ips, 1 - xl), (ipk, xl)):
                cols = pl.ds(pl.multiple_of((side * 4 + z) * OWN, OWN), OWN)
                ref[...] = (ipv[:, cols] + ipr[0, side]) + (ipr[1, side] + ipr[2, side])

    done = set()

    def once(key, ref, sem):
        if key in done:
            return
        done.add(key)
        with scope("w_" + key):
            await_bytes(ref, sem)

    def product(p, s, n, width):
        rows = slice(2 * OFFS[p], 2 * OFFS[p] + 2 * CUTS[p])
        cols = pl.ds(pl.multiple_of(n * width, width), width)
        return rows, cols, jnp.dot(hg[s, rows, :], ogg[:, cols], preferred_element_type=F32)

    def rows_of(p):
        return pl.ds(2 * OFFS[p], 2 * CUTS[p])

    in_parts = set()

    def y_wait(p, s):
        if s == 0 and p in in_parts:
            for k in range(PARTS):
                once(f"y{p}{s}{k}", yrecv.at[s, rows_of(p), pl.ds(k * WIDE, WIDE)], ysp.at[p, k])
        else:
            once(f"y{p}{s}", yrecv.at[s, rows_of(p)], ysr.at[p, s])

    def unit(p, s, part=None):
        m, off = CUTS[p], OFFS[p]
        parts = range(PARTS) if part is None else (part,)
        once(f"hid{p}{s}", hg.at[s, rows_of(p), pl.ds(TOK, 3 * TOK)], hsr.at[p, s])
        for k in parts:
            once(f"og{k}", part_of(3, k), ogr.at[k])
        with scope(f"mm{p}{s}"):

            @pl.loop(parts[0], parts[-1] + 1)
            def _(n):
                rows, cols, got = product(p, s, n, WIDE)
                if s:
                    acc[rows, cols] = got
                else:
                    ysend[s, rows, cols] = got.astype(BF16)

        if s:
            y_wait(p, s - 1)
        if s == 3:
            return
        if s:
            with scope(f"add{p}{s}"):

                @pl.loop(0, REP)
                def _(n):
                    rows, cols = slice(2 * off, 2 * off + 2 * m), pl.ds(pl.multiple_of(n * OWN, OWN), OWN)
                    ysend[s, rows, cols] = (acc[rows, cols] + yrecv[s - 1, rows, cols].astype(F32)).astype(BF16)

        cols = pl.ds(0, COLS) if part is None else pl.ds(part * WIDE, WIDE)
        for start, to in ((2 * off, up), (2 * off + m, down)):
            there = (s, pl.ds(start, m), cols)
            arrived = ysr.at[p, s] if part is None else ysp.at[p, part]
            send(ysend.at[there], yrecv.at[there], yss, arrived, to).start()
        if part is not None:
            in_parts.add(p)

    def out_unit(s):
        m, off = CUTS[OUT], OFFS[OUT]
        once("ogm", ogg.at[pl.ds(TOK, TOK)], ogm)
        once(f"hide{s}", hge.at[s, :, pl.ds(TOK, TOK)], her.at[s])
        with scope(f"mme{s}"):

            @pl.loop(0, PARTS)
            def _(n):
                cols = pl.ds(pl.multiple_of(n * WIDE, WIDE), WIDE)
                got = jnp.dot(hge[s], ogg[0 : 2 * TOK, cols], preferred_element_type=F32)
                if s:
                    ace[:, cols] = got
                else:
                    yse[s, :, cols] = got.astype(BF16)

        if s:
            once(f"ye{s - 1}", yre.at[s - 1], yer.at[s - 1])
            with scope(f"adde{s}"):

                @pl.loop(0, REP)
                def _(n):
                    cols = pl.ds(pl.multiple_of(n * OWN, OWN), OWN)
                    got = ace[:, cols] + yre[s - 1, :, cols].astype(F32)
                    if s < 3:
                        yse[s, :, cols] = got.astype(BF16)
                    else:
                        for i in range(2):
                            acc[2 * off + i * m : 2 * off + (i + 1) * m, cols] = got[2 * i * m : (2 * i + 1) * m]
                            xse[i * m : (i + 1) * m, cols] = got[(2 * i + 1) * m : (2 * i + 2) * m].astype(BF16)

        if s < 3:
            for i, to in enumerate((up, down)):
                there = (s, pl.ds(2 * i * m, 2 * m))
                send(yse.at[there], yre.at[there], yes, yer.at[s], to).start()
        else:
            send(xse, xre, xes, xer, opp).start()

    def adam(p):
        m, off = CUTS[p], OFFS[p]
        if p == OUT:
            once("xe", xre, xer)
        else:
            unit(p, 3)
        if "state" not in done:
            done.add("state")
            for q in (*state_in[:2], *state_in[3:]):
                q.wait()
        with scope(f"adam{p}"):

            @pl.loop(0, REP)
            def _(n):
                cols = pl.ds(pl.multiple_of(n * OWN, OWN), OWN)
                owner_x, owner_z = div(n, 4), rem(n, 4)
                for i, start in enumerate((off, HALF + off)):
                    own_rows, at_rows = slice(2 * off + i * m, 2 * off + (i + 1) * m), slice(start, start + m)
                    last = xre[i * m : (i + 1) * m, cols] if p == OUT else yrecv[2, own_rows, cols]
                    g = acc[own_rows, cols] + last.astype(F32)
                    one = beta_one * fmv[at_rows, cols].astype(F32) + (1.0 - beta_one) * g
                    two = beta_two * smv[at_rows, cols].astype(F32) + (1.0 - beta_two) * g * g
                    o_nf[at_rows, cols] = one.astype(BF16)
                    o_ns[at_rows, cols] = two.astype(BF16)
                    w = ipv[at_rows, cols]
                    hat_one = one * (1.0 / (1.0 - beta_one**INNER_STEP))
                    hat_two = two * (1.0 / (1.0 - beta_two**INNER_STEP))
                    stp[owner_z, owner_x, own_rows, :] = (
                        -inner_rate * (hat_one / (jnp.sqrt(hat_two) + epsilon) + weight_decay * w)
                    ).astype(BF16)

        span = rows_of(p)
        for d in (1, 2, 3):
            there = rem(z + d, 4)
            send(stp.at[there, :, span], rsz.at[3 - d, :, span], rzs, rzr.at[p], column[d - 1]).start()

    def reduce_z(p):
        m, off = CUTS[p], OFFS[p]
        rows, span = slice(2 * off, 2 * off + 2 * m), pl.ds(2 * off, 2 * m)
        once(f"rz{p}", rsz.at[:, :, span], rzr.at[p])
        with scope(f"sum{p}"):
            for ref, inner, side in ((xsend, ips, 1 - xl), (xkeep, ipk, xl)):
                a, b, d, e = (
                    v.astype(F32)
                    for v in (stp[z, side, rows, :], rsz[0, side, rows, :], rsz[1, side, rows, :], rsz[2, side, rows, :])
                )
                change = (a + b) + (d + e)
                for i, start in enumerate((off, HALF + off)):
                    ref[2 * off + i * m : 2 * off + (i + 1) * m, :] = (
                        inner[start : start + m, :] + change[i * m : (i + 1) * m]
                    )
        send(xsend.at[span], xrecv.at[span], rxs, rxr.at[p], beside).start()

    def outer(p):
        m, off = CUTS[p], OFFS[p]
        span = pl.ds(2 * off, 2 * m)
        once(f"rx{p}", xrecv.at[span], rxr.at[p])
        with scope(f"outer{p}"):
            for i, start in enumerate((off, HALF + off)):
                own_rows, at_rows = slice(2 * off + i * m, 2 * off + (i + 1) * m), slice(start, start + m)
                params = opv[at_rows, :]
                delta = params - (xkeep[own_rows, :] + xrecv[own_rows, :]) / REP
                momentum = nesterov * omv[at_rows, :] + delta
                o_nm[at_rows, :] = momentum
                agb[z, xl, own_rows, :] = (params - outer_rate * (delta + nesterov * momentum)).astype(BF16)
        if GATHER[p] == "x":
            give(p, z, xl, axs, axr, beside)
        for to in column:
            give(p, z, xl, azs, azr, to)
        if GATHER[p] != "x":
            give(p, z, xl, axs, axr, beside)
        if GATHER[p] == "d":
            for to in across:
                give(p, z, xl, axs, axr, to)

    def give(p, zz, xx, ss, rs, to):
        here = (zz, xx, rows_of(p))
        send(agb.at[here], agb.at[here], ss, rs.at[p], to).start()

    def pass_on(p):
        if GATHER[p] == "x":
            once(f"ax{p}", agb.at[0, 0, rows_of(p)], axr.at[p])
            for to in column:
                give(p, z, 1 - xl, azs, azr, to)
        else:
            once(f"az{p}", agb.at[pl.ds(0, 3), 0, rows_of(p)], azr.at[p])
            for d in (1, 2, 3):
                give(p, rem(z + d, 4), xl, axs, axr, beside)

    def finish(p):
        m, off = CUTS[p], OFFS[p]
        if GATHER[p] == "x":
            once(f"az{p}", agb.at[pl.ds(0, 3), :, rows_of(p)], azr.at[p])
        else:
            once(f"az{p}", agb.at[pl.ds(0, 3), 0, rows_of(p)], azr.at[p])
            once(f"ax{p}", agb.at[:, 0, rows_of(p)], axr.at[p])
        with scope(f"out{p}"):
            for zz in range(4):
                for xx in range(2):
                    for i, start in enumerate((off, HALF + off)):
                        o_np[start : start + m, (xx * 4 + zz) * OWN : (xx * 4 + zz + 1) * OWN] = agb[
                            zz, xx, 2 * off + i * m : 2 * off + (i + 1) * m, :
                        ]

    def forward(k):
        once(f"ogx{k}", part_of(2, k), ogx.at[k])
        og_pass[k].start()

    run = {
        "out": out_unit, "fwd": forward, "unit": unit, "adam": adam, "rz": reduce_z, "outer": outer,
        "pass": pass_on, "inner": sum_inner, "end": finish,
    }
    for kind, *rest in TASKS:
        run[kind](*rest)

    with scope("drain"):
        await_bytes(ogg.at[pl.ds(0, 3 * TOK)], ogs)
        kept = pl.ds(0, 2 * OFFS[OUT])
        await_bytes(hs.at[:, :, kept], hss)
        await_bytes(ysend.at[:, kept], yss)
        await_bytes(hse, hes)
        await_bytes(yse, yes)
        await_bytes(xse, xes)
        await_bytes(rsz, rzs)
        await_bytes(xsend, rxs)
        for p in range(PIPES):
            x_first = GATHER[p] == "x"
            await_bytes(agb.at[0, 0, rows_of(p)] if x_first else agb.at[:, 0, rows_of(p)], axs)
            await_bytes(agb.at[pl.ds(0, 3), :, rows_of(p)] if x_first else agb.at[pl.ds(0, 3), 0, rows_of(p)], azs)
        await_bytes(ipr, ips_)


def per_device(hidden, out_grad, inner_params, first, second, outer_params, outer_momentum):
    any_ = pl.BlockSpec(memory_space=pl.ANY)
    dma, vmem = pltpu.SemaphoreType.DMA, pltpu.VMEM
    params, momentum, one, two = pl.pallas_call(
        kernel,
        out_shape=(
            vmem((ROWS, COLS), BF16),
            vmem((ROWS, OWN), F32),
            vmem((ROWS, COLS), BF16),
            vmem((ROWS, COLS), BF16),
        ),
        in_specs=[any_] * 7,
        out_specs=(pl.BlockSpec(memory_space=vmem),) * 4,
        scratch_shapes=[
            vmem((8, TOK, 2 * ROWS), BF16),
            vmem((3, YS, ROWS, TOK), BF16),
            vmem((YS, ROWS, 4 * TOK), BF16),
            vmem((4 * TOK, COLS), BF16),
            vmem((ROWS, COLS), F32),
            vmem((3, ROWS, COLS), BF16),
            vmem((3, ROWS, COLS), BF16),
            vmem((ROWS, COLS), F32),
            vmem((ROWS, COLS), BF16),
            vmem((ROWS, COLS), BF16),
            vmem((ROWS, OWN), F32),
            vmem((ROWS, OWN), F32),
            vmem((4, 2, ROWS, OWN), BF16),
            vmem((3, 2, ROWS, OWN), BF16),
            vmem((ROWS, OWN), F32),
            vmem((ROWS, OWN), F32),
            vmem((ROWS, OWN), F32),
            vmem((4, 2, ROWS, OWN), BF16),
            vmem((3, 2, ROWS, OWN), F32),
            vmem((ROWS, OWN), F32),
            vmem((ROWS, OWN), F32),
            vmem((YS, 4 * CUTS[OUT], TOK), BF16),
            vmem((YS, 4 * CUTS[OUT], 2 * TOK), BF16),
            vmem((4 * CUTS[OUT], COLS), F32),
            vmem((3, 4 * CUTS[OUT], COLS), BF16),
            vmem((3, 4 * CUTS[OUT], COLS), BF16),
            vmem((2 * CUTS[OUT], COLS), BF16),
            vmem((2 * CUTS[OUT], COLS), BF16),
            dma((6,)),
            dma((8,)),
            dma,
            dma,
            dma((PARTS,)),
            dma((PARTS,)),
            dma,
            dma((YS,)),
            dma,
            dma((3,)),
            dma,
            dma,
            dma,
            dma((PIPES, YS)),
            dma,
            dma((PIPES, 3)),
            dma((PIPES, PARTS)),
            dma,
            dma((PIPES,)),
            dma,
            dma((PIPES,)),
            dma,
            dma((PIPES,)),
            dma,
            dma((PIPES,)),
            dma,
            dma,
        ],
        compiler_params=pltpu.CompilerParams(
            collective_id=1, has_side_effects=True, vmem_limit_bytes=55_000_000
        ),
        name="step",
    )(hidden, out_grad, inner_params, first, second, outer_params, outer_momentum)
    return params.astype(F32), momentum, one[None], two[None]


def solution(mesh):
    return jax.shard_map(
        per_device,
        mesh=mesh,
        in_specs=(
            P(("rep", "fsdp"), None),
            P(("rep", "fsdp"), None),
            P("rep", "fsdp", None),
            P("rep", "fsdp", None),
            P("rep", "fsdp", None),
            P("fsdp", "rep"),
            P("fsdp", "rep"),
        ),
        out_specs=(
            P("fsdp", None),
            P("fsdp", "rep"),
            P("rep", "fsdp", None),
            P("rep", "fsdp", None),
        ),
        check_vma=False,
    )
```

```python
import functools

import jax
import jax.numpy as jnp
from jax import lax
from jax.experimental import pallas as pl
from jax.experimental.pallas import tpu as pltpu
from jax.sharding import PartitionSpec as P

INNER_STEP = 500

beta_one = 0.9
beta_two = 0.95
epsilon = 1e-08
inner_rate = 0.0004
weight_decay = 0.1
outer_rate = 0.7
nesterov = 0.9

MESH = pl.DeviceIdType.MESH
BF16, F32 = jnp.bfloat16, jnp.float32

CUTS = (48, 48, 32, 16, 48, 32)
OUT = 5
OFFS = tuple(sum(CUTS[:p]) for p in range(len(CUTS)))
PIPES = len(CUTS)
ROWS, COLS, TOK, REP, YS = 448, 2048, 256, 8, 4
HALF = ROWS // 2
OWN = COLS // REP
PARTS = 4
WIDE = COLS // PARTS
LEAVE = (
    (-1, 0), (2, 0), (1, 0), (-1, 1), (0, 0), (-1, 2), (-1, 3), (2, 1), (4, 0), (3, 0), (0, 1), (3, 1), (1, 1),
    (2, 3), (0, 2), (1, 2), (0, 3), (4, 1), (4, 2), (2, 2), (1, 3), (3, 3), (3, 2), (4, 3),
)
TASKS = (
    ("out", 0), ("fwd", 0), ("unit", 1, 0, 0), ("out", 1), ("fwd", 1), ("unit", 2, 0, 1), ("unit", 1, 0, 1),
    ("out", 2), ("unit", 0, 0, 0), ("fwd", 2), ("unit", 0, 0, 2), ("unit", 2, 0, 0), ("unit", 0, 0, 1),
    ("unit", 1, 0, 2), ("unit", 2, 0, 2), ("fwd", 3), ("unit", 2, 0, 3), ("unit", 1, 0, 3), ("unit", 0, 0, 3),
    ("unit", 4, 0), ("unit", 0, 1), ("unit", 1, 1), ("unit", 0, 2), ("out", 3), ("unit", 1, 2), ("unit", 4, 1),
    ("inner",), ("unit", 2, 1), ("adam", 0), ("adam", 1), ("unit", 4, 2), ("rz", 0), ("unit", 3, 0), ("adam", 5),
    ("unit", 2, 2), ("rz", 1), ("outer", 0), ("adam", 4), ("unit", 3, 1), ("adam", 2), ("rz", 5), ("unit", 3, 2),
    ("outer", 1), ("rz", 4), ("outer", 5), ("adam", 3), ("pass", 0), ("rz", 2), ("outer", 4), ("pass", 1),
    ("rz", 3), ("outer", 2), ("end", 1), ("outer", 3), ("pass", 5), ("end", 0), ("pass", 4), ("end", 2), ("end", 3),
    ("end", 5), ("end", 4),
)
GATHER = "xzddxz"


def rem(a, b):
    return lax.rem(a, jnp.int32(b))


def div(a, b):
    return lax.div(a, jnp.int32(b))


def kernel(
    hid, og, ip, fm, sm, op, om,
    o_np, o_nm, o_nf, o_ns,
    hv, hs, hg, ogg, acc, ysend, yrecv, ipv, fmv, smv, opv, omv, stp, rsz, xsend, xkeep, xrecv, agb,
    ipr, ips, ipk, hse, hge, ace, yse, yre, xse, xre,
    ld, ldh, ogs, ogm, ogx, ogr, hes, her, yes, yer, xes, xer,
    hss, hsr, yss, ysr, ysp, rzs, rzr, rxs, rxr, axs, axr, azs, azr,
    ips_, ipr_,
):
    scope = jax.named_scope
    r, f = lax.axis_index("rep"), lax.axis_index("fsdp")
    xl, z = div(r, 4), rem(r, 4)
    y, xh, c = div(f, 4), rem(div(f, 2), 2), rem(f, 2)

    def at(yy, xx, cc):
        return (r, yy * 4 + xx * 2 + cc)

    mate, opp, opp_mate = at(y, xh, 1 - c), at(y, 1 - xh, c), at(y, 1 - xh, 1 - c)
    targets = (mate, opp, opp_mate)
    up, down = at(rem(y + 1, 4), xh, c), at(rem(y + 3, 4), xh, c)
    beside = ((1 - xl) * 4 + z, f)
    column = tuple((xl * 4 + rem(z + d, 4), f) for d in (1, 2, 3))

    def send(src, dst, ss, rs, to):
        q = pltpu.make_async_remote_copy(
            src_ref=src, dst_ref=dst, send_sem=ss, recv_sem=rs, device_id=to, device_id_type=MESH
        )
        return q

    def await_bytes(ref, sem):
        pltpu.make_async_copy(ref, ref, sem).wait()

    og_in = pltpu.make_async_copy(og, ogg.at[pl.ds(0, TOK)], ld.at[0])
    og_in.start()
    chunk_order = ((0, 1), (2, 1), (0, 0), (2, 0), (1, 1), (3, 1), (1, 0), (3, 0))
    loads = {}
    for i, (s, o) in enumerate(chunk_order):
        yy, xx = rem(y + 3 - s + 4, 4), rem(xh + o, 2)
        first = pl.multiple_of((yy * 2 + xx) * (2 * ROWS), 128)
        loads[s, o] = pltpu.make_async_copy(hid.at[:, pl.ds(first, 2 * ROWS)], hv.at[i], ldh.at[i])
        loads[s, o].start()
    state_in = [
        pltpu.make_async_copy(a, b, ld.at[1 + i])
        for i, (a, b) in enumerate(((fm.at[0], fmv), (sm.at[0], smv), (ip.at[0], ipv), (op, opv), (om, omv)))
    ]
    for q in state_in:
        q.start()

    barrier = pltpu.get_barrier_semaphore()
    across = tuple(((1 - xl) * 4 + rem(z + d, 4), f) for d in (1, 2, 3))
    friends = [*targets, up, down, beside, *column] + ([*across] if "d" in GATHER else [])
    for d in friends:
        pl.semaphore_signal(barrier, inc=1, device_id=d, device_id_type=MESH)
    def part_of(source, k):
        return ogg.at[pl.ds(source * TOK, TOK), pl.ds(k * WIDE, WIDE)]

    og_mate = [send(part_of(0, k), part_of(1, k), ogs, ogm, mate) for k in range(PARTS)]
    og_opp = [send(part_of(0, k), part_of(2, k), ogs, ogx.at[k], opp) for k in range(PARTS)]
    og_pass = [send(part_of(2, k), part_of(3, k), ogs, ogr.at[k], mate) for k in range(PARTS)]
    def turn(i):
        s, o = chunk_order[i]
        with scope(f"turn{i}"):
            loads[s, o].wait()
            turned = hv[i].T
            s_down = (2 - s) % 4
            for cc in range(2):
                for p in range(PIPES):
                    m, off = CUTS[p], OFFS[p]
                    top = turned[ROWS * cc + off : ROWS * cc + off + m]
                    low = turned[ROWS * cc + HALF + off : ROWS * cc + HALF + off + m]
                    if p == OUT:

                        @pl.when(c == cc)
                        def _():
                            hge[s, o * m : (o + 1) * m, 0:TOK] = top
                            hge[s_down, (2 + o) * m : (3 + o) * m, 0:TOK] = low

                        @pl.when(c != cc)
                        def _():
                            hse[s, o * m : (o + 1) * m, :] = top
                            hse[s_down, (2 + o) * m : (3 + o) * m, :] = low

                        continue
                    for t, cond in (((1, c == cc), (2, c != cc)) if o else ((None, c == cc), (0, c != cc))):

                        @pl.when(cond)
                        def _(t=t):
                            if t is None:
                                hg[s, 2 * off : 2 * off + m, 0:TOK] = top
                                hg[s_down, 2 * off + m : 2 * off + 2 * m, 0:TOK] = low
                            else:
                                hs[t, s, 2 * off : 2 * off + m, :] = top
                                hs[t, s_down, 2 * off + m : 2 * off + 2 * m, :] = low

    for i in range(4):
        turn(i)
    with scope("greet"):
        pl.semaphore_wait(barrier, len(friends))
    with scope("og_in"):
        og_in.wait()
    og_opp[0].start()
    out_hid = [send(hse.at[s], hge.at[s, :, pl.ds(TOK, TOK)], hes, her.at[s], mate) for s in range(YS)]
    out_hid[0].start()
    for q in og_mate:
        q.start()

    def leave(p, s):
        if p < 0:
            if s:
                og_opp[s].start()
            return
        rows = pl.ds(2 * OFFS[p], 2 * CUTS[p])
        for t in (1, 2, 0):
            send(
                hs.at[t, s, rows], hg.at[s, rows, pl.ds(TOK * (t + 1), TOK)], hss, hsr.at[p, s], targets[t]
            ).start()

    ahead = next(i for i, (p, s) in enumerate(LEAVE) if p >= 0 and s % 2)
    for p, s in LEAVE[:ahead]:
        leave(p, s)
    for i in range(4, 8):
        turn(i)
    for q in out_hid[1:]:
        q.start()
    for p, s in LEAVE[ahead:]:
        leave(p, s)

    state_in[2].wait()
    for d in (1, 2, 3):
        there = rem(z + d, 4)
        for side in range(2):
            cols = pl.ds(pl.multiple_of((side * 4 + there) * OWN, OWN), OWN)
            q = send(ipv.at[:, cols], ipr.at[3 - d, side], ips_, ipr_, column[d - 1])
            q.start()

    def sum_inner():
        once("ip", ipr, ipr_)
        with scope("sum_ip"):
            for ref, side in ((ips, 1 - xl), (ipk, xl)):
                cols = pl.ds(pl.multiple_of((side * 4 + z) * OWN, OWN), OWN)
                ref[...] = (ipv[:, cols] + ipr[0, side]) + (ipr[1, side] + ipr[2, side])

    done = set()

    def once(key, ref, sem):
        if key in done:
            return
        done.add(key)
        with scope("w_" + key):
            await_bytes(ref, sem)

    def product(p, s, n, width):
        rows = slice(2 * OFFS[p], 2 * OFFS[p] + 2 * CUTS[p])
        cols = pl.ds(pl.multiple_of(n * width, width), width)
        return rows, cols, jnp.dot(hg[s, rows, :], ogg[:, cols], preferred_element_type=F32)

    def rows_of(p):
        return pl.ds(2 * OFFS[p], 2 * CUTS[p])

    in_parts = set()

    def y_wait(p, s):
        if s == 0 and p in in_parts:
            for k in range(PARTS):
                once(f"y{p}{s}{k}", yrecv.at[s, rows_of(p), pl.ds(k * WIDE, WIDE)], ysp.at[p, k])
        else:
            once(f"y{p}{s}", yrecv.at[s, rows_of(p)], ysr.at[p, s])

    def unit(p, s, part=None):
        m, off = CUTS[p], OFFS[p]
        parts = range(PARTS) if part is None else (part,)
        once(f"hid{p}{s}", hg.at[s, rows_of(p), pl.ds(TOK, 3 * TOK)], hsr.at[p, s])
        for k in parts:
            once(f"og{k}", part_of(3, k), ogr.at[k])
        with scope(f"mm{p}{s}"):

            @pl.loop(parts[0], parts[-1] + 1)
            def _(n):
                rows, cols, got = product(p, s, n, WIDE)
                if s:
                    acc[rows, cols] = got
                else:
                    ysend[s, rows, cols] = got.astype(BF16)

        if s:
            y_wait(p, s - 1)
        if s == 3:
            return
        if s:
            with scope(f"add{p}{s}"):

                @pl.loop(0, REP)
                def _(n):
                    rows, cols = slice(2 * off, 2 * off + 2 * m), pl.ds(pl.multiple_of(n * OWN, OWN), OWN)
                    ysend[s, rows, cols] = (acc[rows, cols] + yrecv[s - 1, rows, cols].astype(F32)).astype(BF16)

        cols = pl.ds(0, COLS) if part is None else pl.ds(part * WIDE, WIDE)
        for start, to in ((2 * off, up), (2 * off + m, down)):
            there = (s, pl.ds(start, m), cols)
            arrived = ysr.at[p, s] if part is None else ysp.at[p, part]
            send(ysend.at[there], yrecv.at[there], yss, arrived, to).start()
        if part is not None:
            in_parts.add(p)

    def out_unit(s):
        m, off = CUTS[OUT], OFFS[OUT]
        once("ogm", ogg.at[pl.ds(TOK, TOK)], ogm)
        once(f"hide{s}", hge.at[s, :, pl.ds(TOK, TOK)], her.at[s])
        with scope(f"mme{s}"):

            @pl.loop(0, PARTS)
            def _(n):
                cols = pl.ds(pl.multiple_of(n * WIDE, WIDE), WIDE)
                got = jnp.dot(hge[s], ogg[0 : 2 * TOK, cols], preferred_element_type=F32)
                if s:
                    ace[:, cols] = got
                else:
                    yse[s, :, cols] = got.astype(BF16)

        if s:
            once(f"ye{s - 1}", yre.at[s - 1], yer.at[s - 1])
            with scope(f"adde{s}"):

                @pl.loop(0, REP)
                def _(n):
                    cols = pl.ds(pl.multiple_of(n * OWN, OWN), OWN)
                    got = ace[:, cols] + yre[s - 1, :, cols].astype(F32)
                    if s < 3:
                        yse[s, :, cols] = got.astype(BF16)
                    else:
                        for i in range(2):
                            acc[2 * off + i * m : 2 * off + (i + 1) * m, cols] = got[2 * i * m : (2 * i + 1) * m]
                            xse[i * m : (i + 1) * m, cols] = got[(2 * i + 1) * m : (2 * i + 2) * m].astype(BF16)

        if s < 3:
            for i, to in enumerate((up, down)):
                there = (s, pl.ds(2 * i * m, 2 * m))
                send(yse.at[there], yre.at[there], yes, yer.at[s], to).start()
        else:
            send(xse, xre, xes, xer, opp).start()

    def adam(p):
        m, off = CUTS[p], OFFS[p]
        if p == OUT:
            once("xe", xre, xer)
        else:
            unit(p, 3)
        if "state" not in done:
            done.add("state")
            for q in (*state_in[:2], *state_in[3:]):
                q.wait()
        with scope(f"adam{p}"):

            @pl.loop(0, REP)
            def _(n):
                cols = pl.ds(pl.multiple_of(n * OWN, OWN), OWN)
                owner_x, owner_z = div(n, 4), rem(n, 4)
                for i, start in enumerate((off, HALF + off)):
                    own_rows, at_rows = slice(2 * off + i * m, 2 * off + (i + 1) * m), slice(start, start + m)
                    last = xre[i * m : (i + 1) * m, cols] if p == OUT else yrecv[2, own_rows, cols]
                    g = acc[own_rows, cols] + last.astype(F32)
                    one = beta_one * fmv[at_rows, cols].astype(F32) + (1.0 - beta_one) * g
                    two = beta_two * smv[at_rows, cols].astype(F32) + (1.0 - beta_two) * g * g
                    o_nf[at_rows, cols] = one.astype(BF16)
                    o_ns[at_rows, cols] = two.astype(BF16)
                    w = ipv[at_rows, cols]
                    hat_one = one * (1.0 / (1.0 - beta_one**INNER_STEP))
                    hat_two = two * (1.0 / (1.0 - beta_two**INNER_STEP))
                    stp[owner_z, owner_x, own_rows, :] = (
                        -inner_rate * (hat_one / (jnp.sqrt(hat_two) + epsilon) + weight_decay * w)
                    ).astype(BF16)

        span = rows_of(p)
        for d in (1, 2, 3):
            there = rem(z + d, 4)
            send(stp.at[there, :, span], rsz.at[3 - d, :, span], rzs, rzr.at[p], column[d - 1]).start()

    def reduce_z(p):
        m, off = CUTS[p], OFFS[p]
        rows, span = slice(2 * off, 2 * off + 2 * m), pl.ds(2 * off, 2 * m)
        once(f"rz{p}", rsz.at[:, :, span], rzr.at[p])
        with scope(f"sum{p}"):
            for ref, inner, side in ((xsend, ips, 1 - xl), (xkeep, ipk, xl)):
                a, b, d, e = (
                    v.astype(F32)
                    for v in (stp[z, side, rows, :], rsz[0, side, rows, :], rsz[1, side, rows, :], rsz[2, side, rows, :])
                )
                change = (a + b) + (d + e)
                for i, start in enumerate((off, HALF + off)):
                    ref[2 * off + i * m : 2 * off + (i + 1) * m, :] = (
                        inner[start : start + m, :] + change[i * m : (i + 1) * m]
                    )
        send(xsend.at[span], xrecv.at[span], rxs, rxr.at[p], beside).start()

    def outer(p):
        m, off = CUTS[p], OFFS[p]
        span = pl.ds(2 * off, 2 * m)
        once(f"rx{p}", xrecv.at[span], rxr.at[p])
        with scope(f"outer{p}"):
            for i, start in enumerate((off, HALF + off)):
                own_rows, at_rows = slice(2 * off + i * m, 2 * off + (i + 1) * m), slice(start, start + m)
                params = opv[at_rows, :]
                delta = params - (xkeep[own_rows, :] + xrecv[own_rows, :]) / REP
                momentum = nesterov * omv[at_rows, :] + delta
                o_nm[at_rows, :] = momentum
                agb[z, xl, own_rows, :] = (params - outer_rate * (delta + nesterov * momentum)).astype(BF16)
        if GATHER[p] == "x":
            give(p, z, xl, axs, axr, beside)
        for to in column:
            give(p, z, xl, azs, azr, to)
        if GATHER[p] != "x":
            give(p, z, xl, axs, axr, beside)
        if GATHER[p] == "d":
            for to in across:
                give(p, z, xl, axs, axr, to)

    def give(p, zz, xx, ss, rs, to):
        here = (zz, xx, rows_of(p))
        send(agb.at[here], agb.at[here], ss, rs.at[p], to).start()

    def pass_on(p):
        if GATHER[p] == "x":
            once(f"ax{p}", agb.at[0, 0, rows_of(p)], axr.at[p])
            for to in column:
                give(p, z, 1 - xl, azs, azr, to)
        else:
            once(f"az{p}", agb.at[pl.ds(0, 3), 0, rows_of(p)], azr.at[p])
            for d in (1, 2, 3):
                give(p, rem(z + d, 4), xl, axs, axr, beside)

    def finish(p):
        m, off = CUTS[p], OFFS[p]
        if GATHER[p] == "x":
            once(f"az{p}", agb.at[pl.ds(0, 3), :, rows_of(p)], azr.at[p])
        else:
            once(f"az{p}", agb.at[pl.ds(0, 3), 0, rows_of(p)], azr.at[p])
            once(f"ax{p}", agb.at[:, 0, rows_of(p)], axr.at[p])
        with scope(f"out{p}"):
            for zz in range(4):
                for xx in range(2):
                    for i, start in enumerate((off, HALF + off)):
                        o_np[start : start + m, (xx * 4 + zz) * OWN : (xx * 4 + zz + 1) * OWN] = agb[
                            zz, xx, 2 * off + i * m : 2 * off + (i + 1) * m, :
                        ]

    def forward(k):
        once(f"ogx{k}", part_of(2, k), ogx.at[k])
        og_pass[k].start()

    run = {
        "out": out_unit, "fwd": forward, "unit": unit, "adam": adam, "rz": reduce_z, "outer": outer,
        "pass": pass_on, "inner": sum_inner, "end": finish,
    }
    for kind, *rest in TASKS:
        run[kind](*rest)

    with scope("drain"):
        await_bytes(ogg.at[pl.ds(0, 3 * TOK)], ogs)
        kept = pl.ds(0, 2 * OFFS[OUT])
        await_bytes(hs.at[:, :, kept], hss)
        await_bytes(ysend.at[:, kept], yss)
        await_bytes(hse, hes)
        await_bytes(yse, yes)
        await_bytes(xse, xes)
        await_bytes(rsz, rzs)
        await_bytes(xsend, rxs)
        for p in range(PIPES):
            x_first = GATHER[p] == "x"
            await_bytes(agb.at[0, 0, rows_of(p)] if x_first else agb.at[:, 0, rows_of(p)], axs)
            await_bytes(agb.at[pl.ds(0, 3), :, rows_of(p)] if x_first else agb.at[pl.ds(0, 3), 0, rows_of(p)], azs)
        await_bytes(ipr, ips_)


SLABS = 7


def write_out(params, momentum, one, two, o_params, o_momentum, o_one, o_two, wide, sem):
    copies = [
        pltpu.make_async_copy(a, b, sem.at[i])
        for i, (a, b) in enumerate(((one, o_one), (two, o_two), (momentum, o_momentum)))
    ]
    for q in copies:
        q.start()
    for k in range(SLABS):
        rows = pl.ds(k * (ROWS // SLABS), ROWS // SLABS)
        wide[rows, :] = params[rows, :].astype(F32)
        q = pltpu.make_async_copy(wide.at[rows], o_params.at[rows], sem.at[3 + k])
        q.start()
        copies.append(q)
    for q in copies:
        q.wait()


def per_device(hidden, out_grad, inner_params, first, second, outer_params, outer_momentum):
    any_ = pl.BlockSpec(memory_space=pl.ANY)
    dma, vmem = pltpu.SemaphoreType.DMA, pltpu.VMEM
    params, momentum, one, two = pl.pallas_call(
        kernel,
        out_shape=(
            vmem((ROWS, COLS), BF16),
            vmem((ROWS, OWN), F32),
            vmem((ROWS, COLS), BF16),
            vmem((ROWS, COLS), BF16),
        ),
        in_specs=[any_] * 7,
        out_specs=(pl.BlockSpec(memory_space=vmem),) * 4,
        scratch_shapes=[
            vmem((8, TOK, 2 * ROWS), BF16),
            vmem((3, YS, ROWS, TOK), BF16),
            vmem((YS, ROWS, 4 * TOK), BF16),
            vmem((4 * TOK, COLS), BF16),
            vmem((ROWS, COLS), F32),
            vmem((3, ROWS, COLS), BF16),
            vmem((3, ROWS, COLS), BF16),
            vmem((ROWS, COLS), F32),
            vmem((ROWS, COLS), BF16),
            vmem((ROWS, COLS), BF16),
            vmem((ROWS, OWN), F32),
            vmem((ROWS, OWN), F32),
            vmem((4, 2, ROWS, OWN), BF16),
            vmem((3, 2, ROWS, OWN), BF16),
            vmem((ROWS, OWN), F32),
            vmem((ROWS, OWN), F32),
            vmem((ROWS, OWN), F32),
            vmem((4, 2, ROWS, OWN), BF16),
            vmem((3, 2, ROWS, OWN), F32),
            vmem((ROWS, OWN), F32),
            vmem((ROWS, OWN), F32),
            vmem((YS, 4 * CUTS[OUT], TOK), BF16),
            vmem((YS, 4 * CUTS[OUT], 2 * TOK), BF16),
            vmem((4 * CUTS[OUT], COLS), F32),
            vmem((3, 4 * CUTS[OUT], COLS), BF16),
            vmem((3, 4 * CUTS[OUT], COLS), BF16),
            vmem((2 * CUTS[OUT], COLS), BF16),
            vmem((2 * CUTS[OUT], COLS), BF16),
            dma((6,)),
            dma((8,)),
            dma,
            dma,
            dma((PARTS,)),
            dma((PARTS,)),
            dma,
            dma((YS,)),
            dma,
            dma((3,)),
            dma,
            dma,
            dma,
            dma((PIPES, YS)),
            dma,
            dma((PIPES, 3)),
            dma((PIPES, PARTS)),
            dma,
            dma((PIPES,)),
            dma,
            dma((PIPES,)),
            dma,
            dma((PIPES,)),
            dma,
            dma((PIPES,)),
            dma,
            dma,
        ],
        compiler_params=pltpu.CompilerParams(
            collective_id=1, has_side_effects=True, vmem_limit_bytes=55_000_000
        ),
        name="step",
    )(hidden, out_grad, inner_params, first, second, outer_params, outer_momentum)
    params, momentum, one, two = pl.pallas_call(
        write_out,
        out_shape=(
            jax.ShapeDtypeStruct((ROWS, COLS), F32),
            jax.ShapeDtypeStruct((ROWS, OWN), F32),
            jax.ShapeDtypeStruct((ROWS, COLS), BF16),
            jax.ShapeDtypeStruct((ROWS, COLS), BF16),
        ),
        in_specs=[pl.BlockSpec(memory_space=vmem)] * 4,
        out_specs=(any_,) * 4,
        scratch_shapes=[vmem((ROWS, COLS), F32), dma((3 + SLABS,))],
        compiler_params=pltpu.CompilerParams(vmem_limit_bytes=8_000_000),
        name="write",
    )(params, momentum, one, two)
    return params, momentum, one[None], two[None]


def solution(mesh):
    return jax.shard_map(
        per_device,
        mesh=mesh,
        in_specs=(
            P(("rep", "fsdp"), None),
            P(("rep", "fsdp"), None),
            P("rep", "fsdp", None),
            P("rep", "fsdp", None),
            P("rep", "fsdp", None),
            P("fsdp", "rep"),
            P("fsdp", "rep"),
        ),
        out_specs=(
            P("fsdp", None),
            P("fsdp", "rep"),
            P("rep", "fsdp", None),
            P("rep", "fsdp", None),
        ),
        check_vma=False,
    )
```

```python
import functools

import jax
import jax.numpy as jnp
from jax import lax
from jax.experimental import pallas as pl
from jax.experimental.pallas import tpu as pltpu
from jax.sharding import PartitionSpec as P

INNER_STEP = 500

beta_one = 0.9
beta_two = 0.95
epsilon = 1e-08
inner_rate = 0.0004
weight_decay = 0.1
outer_rate = 0.7
nesterov = 0.9

MESH = pl.DeviceIdType.MESH
BF16, F32 = jnp.bfloat16, jnp.float32

CUTS = (48, 48, 32, 16, 48, 32)
OUT = 5
OFFS = tuple(sum(CUTS[:p]) for p in range(len(CUTS)))
PIPES = len(CUTS)
ROWS, COLS, TOK, REP, YS = 448, 2048, 256, 8, 4
HALF = ROWS // 2
OWN = COLS // REP
PARTS = 4
WIDE = COLS // PARTS
LEAVE = (
    (-1, 0), (2, 0), (1, 0), (-1, 1), (0, 0), (-1, 2), (-1, 3), (2, 1), (4, 0), (3, 0), (0, 1), (3, 1), (1, 1),
    (2, 3), (0, 2), (1, 2), (0, 3), (4, 1), (4, 2), (2, 2), (1, 3), (3, 3), (3, 2), (4, 3),
)
TASKS = (
    ("out", 0), ("fwd", 0), ("unit", 1, 0, 0), ("out", 1), ("fwd", 1), ("unit", 2, 0, 1), ("unit", 1, 0, 1),
    ("out", 2), ("unit", 0, 0, 0), ("fwd", 2), ("unit", 0, 0, 2), ("unit", 2, 0, 0), ("unit", 0, 0, 1),
    ("unit", 1, 0, 2), ("unit", 2, 0, 2), ("fwd", 3), ("unit", 2, 0, 3), ("unit", 1, 0, 3), ("unit", 0, 0, 3),
    ("unit", 4, 0), ("unit", 0, 1), ("unit", 1, 1), ("unit", 0, 2), ("out", 3), ("unit", 1, 2), ("unit", 4, 1),
    ("inner",), ("unit", 2, 1), ("adam", 0), ("adam", 1), ("unit", 4, 2), ("rz", 0), ("unit", 3, 0), ("adam", 5),
    ("unit", 2, 2), ("rz", 1), ("outer", 0), ("adam", 4), ("unit", 3, 1), ("adam", 2), ("rz", 5), ("unit", 3, 2),
    ("outer", 1), ("outer", 5), ("adam", 3), ("pass", 0), ("rz", 2), ("outer", 4), ("pass", 1), ("outer", 2),
    ("end", 1), ("outer", 3), ("pass", 5), ("end", 0), ("pass", 4), ("end", 2), ("end", 3), ("end", 5), ("end", 4),
)
SUM = "zzzddz"
GATHER = "xzddxz"


def rem(a, b):
    return lax.rem(a, jnp.int32(b))


def div(a, b):
    return lax.div(a, jnp.int32(b))


def kernel(
    hid, og, ip, fm, sm, op, om,
    o_np, o_nm, o_nf, o_ns,
    hv, hs, hg, ogg, acc, ysend, yrecv, ipv, fmv, smv, opv, omv, stp, rsz, xsend, xkeep, xrecv, agb,
    ipr, ips, ipk, ipx, xrb, hse, hge, ace, yse, yre, xse, xre,
    ld, ldh, ogs, ogm, ogx, ogr, hes, her, yes, yer, xes, xer,
    hss, hsr, yss, ysr, ysp, rzs, rzr, rxs, rxr, axs, axr, azs, azr,
    ips_, ipr_, ixs, ixr,
):
    scope = jax.named_scope
    r, f = lax.axis_index("rep"), lax.axis_index("fsdp")
    xl, z = div(r, 4), rem(r, 4)
    y, xh, c = div(f, 4), rem(div(f, 2), 2), rem(f, 2)

    def at(yy, xx, cc):
        return (r, yy * 4 + xx * 2 + cc)

    mate, opp, opp_mate = at(y, xh, 1 - c), at(y, 1 - xh, c), at(y, 1 - xh, 1 - c)
    targets = (mate, opp, opp_mate)
    up, down = at(rem(y + 1, 4), xh, c), at(rem(y + 3, 4), xh, c)
    beside = ((1 - xl) * 4 + z, f)
    column = tuple((xl * 4 + rem(z + d, 4), f) for d in (1, 2, 3))

    def send(src, dst, ss, rs, to):
        q = pltpu.make_async_remote_copy(
            src_ref=src, dst_ref=dst, send_sem=ss, recv_sem=rs, device_id=to, device_id_type=MESH
        )
        return q

    def await_bytes(ref, sem):
        pltpu.make_async_copy(ref, ref, sem).wait()

    og_in = pltpu.make_async_copy(og, ogg.at[pl.ds(0, TOK)], ld.at[0])
    og_in.start()
    chunk_order = ((0, 1), (2, 1), (0, 0), (2, 0), (1, 1), (3, 1), (1, 0), (3, 0))
    loads = {}
    for i, (s, o) in enumerate(chunk_order):
        yy, xx = rem(y + 3 - s + 4, 4), rem(xh + o, 2)
        first = pl.multiple_of((yy * 2 + xx) * (2 * ROWS), 128)
        loads[s, o] = pltpu.make_async_copy(hid.at[:, pl.ds(first, 2 * ROWS)], hv.at[i], ldh.at[i])
        loads[s, o].start()
    state_in = [
        pltpu.make_async_copy(a, b, ld.at[1 + i])
        for i, (a, b) in enumerate(((fm.at[0], fmv), (sm.at[0], smv), (ip.at[0], ipv), (op, opv), (om, omv)))
    ]
    for q in state_in:
        q.start()

    barrier = pltpu.get_barrier_semaphore()
    across = tuple(((1 - xl) * 4 + rem(z + d, 4), f) for d in (1, 2, 3))
    friends = [*targets, up, down, beside, *column] + ([*across] if "d" in SUM + GATHER else [])
    for d in friends:
        pl.semaphore_signal(barrier, inc=1, device_id=d, device_id_type=MESH)
    def part_of(source, k):
        return ogg.at[pl.ds(source * TOK, TOK), pl.ds(k * WIDE, WIDE)]

    og_mate = [send(part_of(0, k), part_of(1, k), ogs, ogm, mate) for k in range(PARTS)]
    og_opp = [send(part_of(0, k), part_of(2, k), ogs, ogx.at[k], opp) for k in range(PARTS)]
    og_pass = [send(part_of(2, k), part_of(3, k), ogs, ogr.at[k], mate) for k in range(PARTS)]
    def turn(i):
        s, o = chunk_order[i]
        with scope(f"turn{i}"):
            loads[s, o].wait()
            turned = hv[i].T
            s_down = (2 - s) % 4
            for cc in range(2):
                for p in range(PIPES):
                    m, off = CUTS[p], OFFS[p]
                    top = turned[ROWS * cc + off : ROWS * cc + off + m]
                    low = turned[ROWS * cc + HALF + off : ROWS * cc + HALF + off + m]
                    if p == OUT:

                        @pl.when(c == cc)
                        def _():
                            hge[s, o * m : (o + 1) * m, 0:TOK] = top
                            hge[s_down, (2 + o) * m : (3 + o) * m, 0:TOK] = low

                        @pl.when(c != cc)
                        def _():
                            hse[s, o * m : (o + 1) * m, :] = top
                            hse[s_down, (2 + o) * m : (3 + o) * m, :] = low

                        continue
                    for t, cond in (((1, c == cc), (2, c != cc)) if o else ((None, c == cc), (0, c != cc))):

                        @pl.when(cond)
                        def _(t=t):
                            if t is None:
                                hg[s, 2 * off : 2 * off + m, 0:TOK] = top
                                hg[s_down, 2 * off + m : 2 * off + 2 * m, 0:TOK] = low
                            else:
                                hs[t, s, 2 * off : 2 * off + m, :] = top
                                hs[t, s_down, 2 * off + m : 2 * off + 2 * m, :] = low

    for i in range(4):
        turn(i)
    with scope("greet"):
        pl.semaphore_wait(barrier, len(friends))
    with scope("og_in"):
        og_in.wait()
    og_opp[0].start()
    out_hid = [send(hse.at[s], hge.at[s, :, pl.ds(TOK, TOK)], hes, her.at[s], mate) for s in range(YS)]
    out_hid[0].start()
    for q in og_mate:
        q.start()

    def leave(p, s):
        if p < 0:
            if s:
                og_opp[s].start()
            return
        rows = pl.ds(2 * OFFS[p], 2 * CUTS[p])
        for t in (1, 2, 0):
            send(
                hs.at[t, s, rows], hg.at[s, rows, pl.ds(TOK * (t + 1), TOK)], hss, hsr.at[p, s], targets[t]
            ).start()

    ahead = next(i for i, (p, s) in enumerate(LEAVE) if p >= 0 and s % 2)
    for p, s in LEAVE[:ahead]:
        leave(p, s)
    for i in range(4, 8):
        turn(i)
    for q in out_hid[1:]:
        q.start()
    for p, s in LEAVE[ahead:]:
        leave(p, s)

    state_in[2].wait()
    for d in (1, 2, 3):
        there = rem(z + d, 4)
        for side in range(2):
            cols = pl.ds(pl.multiple_of((side * 4 + there) * OWN, OWN), OWN)
            q = send(ipv.at[:, cols], ipr.at[3 - d, side], ips_, ipr_, column[d - 1])
            q.start()

    def sum_inner():
        once("ip", ipr, ipr_)
        with scope("sum_ip"):
            for ref, side in ((ips, 1 - xl), (ipk, xl)):
                cols = pl.ds(pl.multiple_of((side * 4 + z) * OWN, OWN), OWN)
                ref[...] = (ipv[:, cols] + ipr[0, side]) + (ipr[1, side] + ipr[2, side])
        for p in range(PIPES):
            if SUM[p] == "d":
                for start in (OFFS[p], HALF + OFFS[p]):
                    rows = pl.ds(start, CUTS[p])
                    send(ips.at[rows], ipx.at[rows], ixs, ixr.at[p], beside).start()

    done = set()

    def once(key, ref, sem):
        if key in done:
            return
        done.add(key)
        with scope("w_" + key):
            await_bytes(ref, sem)

    def product(p, s, n, width):
        rows = slice(2 * OFFS[p], 2 * OFFS[p] + 2 * CUTS[p])
        cols = pl.ds(pl.multiple_of(n * width, width), width)
        return rows, cols, jnp.dot(hg[s, rows, :], ogg[:, cols], preferred_element_type=F32)

    def rows_of(p):
        return pl.ds(2 * OFFS[p], 2 * CUTS[p])

    in_parts = set()

    def y_wait(p, s):
        if s == 0 and p in in_parts:
            for k in range(PARTS):
                once(f"y{p}{s}{k}", yrecv.at[s, rows_of(p), pl.ds(k * WIDE, WIDE)], ysp.at[p, k])
        else:
            once(f"y{p}{s}", yrecv.at[s, rows_of(p)], ysr.at[p, s])

    def unit(p, s, part=None):
        m, off = CUTS[p], OFFS[p]
        parts = range(PARTS) if part is None else (part,)
        once(f"hid{p}{s}", hg.at[s, rows_of(p), pl.ds(TOK, 3 * TOK)], hsr.at[p, s])
        for k in parts:
            once(f"og{k}", part_of(3, k), ogr.at[k])
        with scope(f"mm{p}{s}"):

            @pl.loop(parts[0], parts[-1] + 1)
            def _(n):
                rows, cols, got = product(p, s, n, WIDE)
                if s:
                    acc[rows, cols] = got
                else:
                    ysend[s, rows, cols] = got.astype(BF16)

        if s:
            y_wait(p, s - 1)
        if s == 3:
            return
        if s:
            with scope(f"add{p}{s}"):

                @pl.loop(0, REP)
                def _(n):
                    rows, cols = slice(2 * off, 2 * off + 2 * m), pl.ds(pl.multiple_of(n * OWN, OWN), OWN)
                    ysend[s, rows, cols] = (acc[rows, cols] + yrecv[s - 1, rows, cols].astype(F32)).astype(BF16)

        cols = pl.ds(0, COLS) if part is None else pl.ds(part * WIDE, WIDE)
        for start, to in ((2 * off, up), (2 * off + m, down)):
            there = (s, pl.ds(start, m), cols)
            arrived = ysr.at[p, s] if part is None else ysp.at[p, part]
            send(ysend.at[there], yrecv.at[there], yss, arrived, to).start()
        if part is not None:
            in_parts.add(p)

    def out_unit(s):
        m, off = CUTS[OUT], OFFS[OUT]
        once("ogm", ogg.at[pl.ds(TOK, TOK)], ogm)
        once(f"hide{s}", hge.at[s, :, pl.ds(TOK, TOK)], her.at[s])
        with scope(f"mme{s}"):

            @pl.loop(0, PARTS)
            def _(n):
                cols = pl.ds(pl.multiple_of(n * WIDE, WIDE), WIDE)
                got = jnp.dot(hge[s], ogg[0 : 2 * TOK, cols], preferred_element_type=F32)
                if s:
                    ace[:, cols] = got
                else:
                    yse[s, :, cols] = got.astype(BF16)

        if s:
            once(f"ye{s - 1}", yre.at[s - 1], yer.at[s - 1])
            with scope(f"adde{s}"):

                @pl.loop(0, REP)
                def _(n):
                    cols = pl.ds(pl.multiple_of(n * OWN, OWN), OWN)
                    got = ace[:, cols] + yre[s - 1, :, cols].astype(F32)
                    if s < 3:
                        yse[s, :, cols] = got.astype(BF16)
                    else:
                        for i in range(2):
                            acc[2 * off + i * m : 2 * off + (i + 1) * m, cols] = got[2 * i * m : (2 * i + 1) * m]
                            xse[i * m : (i + 1) * m, cols] = got[(2 * i + 1) * m : (2 * i + 2) * m].astype(BF16)

        if s < 3:
            for i, to in enumerate((up, down)):
                there = (s, pl.ds(2 * i * m, 2 * m))
                send(yse.at[there], yre.at[there], yes, yer.at[s], to).start()
        else:
            send(xse, xre, xes, xer, opp).start()

    def adam(p):
        m, off = CUTS[p], OFFS[p]
        if p == OUT:
            once("xe", xre, xer)
        else:
            unit(p, 3)
        if "state" not in done:
            done.add("state")
            for q in (*state_in[:2], *state_in[3:]):
                q.wait()
        with scope(f"adam{p}"):

            @pl.loop(0, REP)
            def _(n):
                cols = pl.ds(pl.multiple_of(n * OWN, OWN), OWN)
                owner_x, owner_z = div(n, 4), rem(n, 4)
                for i, start in enumerate((off, HALF + off)):
                    own_rows, at_rows = slice(2 * off + i * m, 2 * off + (i + 1) * m), slice(start, start + m)
                    last = xre[i * m : (i + 1) * m, cols] if p == OUT else yrecv[2, own_rows, cols]
                    g = acc[own_rows, cols] + last.astype(F32)
                    one = beta_one * fmv[at_rows, cols].astype(F32) + (1.0 - beta_one) * g
                    two = beta_two * smv[at_rows, cols].astype(F32) + (1.0 - beta_two) * g * g
                    o_nf[at_rows, cols] = one.astype(BF16)
                    o_ns[at_rows, cols] = two.astype(BF16)
                    w = ipv[at_rows, cols]
                    hat_one = one * (1.0 / (1.0 - beta_one**INNER_STEP))
                    hat_two = two * (1.0 / (1.0 - beta_two**INNER_STEP))
                    stp[owner_z, owner_x, own_rows, :] = (
                        -inner_rate * (hat_one / (jnp.sqrt(hat_two) + epsilon) + weight_decay * w)
                    ).astype(BF16)

        span = rows_of(p)
        for d in (1, 2, 3):
            there = rem(z + d, 4)
            if SUM[p] == "z":
                send(stp.at[there, :, span], rsz.at[3 - d, :, span], rzs, rzr.at[p], column[d - 1]).start()
            else:
                send(stp.at[there, xl, span], rsz.at[3 - d, 0, span], rzs, rzr.at[p], column[d - 1]).start()
                send(stp.at[there, 1 - xl, span], rsz.at[3 - d, 1, span], rzs, rzr.at[p], across[d - 1]).start()
        if SUM[p] == "d":
            send(stp.at[z, 1 - xl, span], xrb.at[span], rxs, rxr.at[p], beside).start()

    def reduce_z(p):
        m, off = CUTS[p], OFFS[p]
        rows, span = slice(2 * off, 2 * off + 2 * m), pl.ds(2 * off, 2 * m)
        once(f"rz{p}", rsz.at[:, :, span], rzr.at[p])
        with scope(f"sum{p}"):
            for ref, inner, side in ((xsend, ips, 1 - xl), (xkeep, ipk, xl)):
                a, b, d, e = (
                    v.astype(F32)
                    for v in (stp[z, side, rows, :], rsz[0, side, rows, :], rsz[1, side, rows, :], rsz[2, side, rows, :])
                )
                change = (a + b) + (d + e)
                for i, start in enumerate((off, HALF + off)):
                    ref[2 * off + i * m : 2 * off + (i + 1) * m, :] = (
                        inner[start : start + m, :] + change[i * m : (i + 1) * m]
                    )
        send(xsend.at[span], xrecv.at[span], rxs, rxr.at[p], beside).start()

    def outer(p):
        m, off = CUTS[p], OFFS[p]
        span = pl.ds(2 * off, 2 * m)
        if SUM[p] == "z":
            once(f"rx{p}", xrecv.at[span], rxr.at[p])
        else:
            once(f"rz{p}", rsz.at[:, :, span], rzr.at[p])
            once(f"rx{p}", xrb.at[span], rxr.at[p])
            once(f"ix{p}", ipx.at[span], ixr.at[p])
        with scope(f"outer{p}"):
            for i, start in enumerate((off, HALF + off)):
                own_rows, at_rows = slice(2 * off + i * m, 2 * off + (i + 1) * m), slice(start, start + m)
                params = opv[at_rows, :]
                if SUM[p] == "z":
                    total = xkeep[own_rows, :] + xrecv[own_rows, :]
                else:
                    change = stp[z, xl, own_rows, :].astype(F32) + xrb[own_rows, :].astype(F32)
                    for k in range(3):
                        change = change + (rsz[k, 0, own_rows, :].astype(F32) + rsz[k, 1, own_rows, :].astype(F32))
                    total = (ipk[at_rows, :] + ipx[at_rows, :]) + change
                delta = params - total / REP
                momentum = nesterov * omv[at_rows, :] + delta
                o_nm[at_rows, :] = momentum
                agb[z, xl, own_rows, :] = (params - outer_rate * (delta + nesterov * momentum)).astype(BF16)
        if GATHER[p] == "x":
            give(p, z, xl, axs, axr, beside)
        for to in column:
            give(p, z, xl, azs, azr, to)
        if GATHER[p] != "x":
            give(p, z, xl, axs, axr, beside)
        if GATHER[p] == "d":
            for to in across:
                give(p, z, xl, axs, axr, to)

    def give(p, zz, xx, ss, rs, to):
        here = (zz, xx, rows_of(p))
        send(agb.at[here], agb.at[here], ss, rs.at[p], to).start()

    def pass_on(p):
        if GATHER[p] == "x":
            once(f"ax{p}", agb.at[0, 0, rows_of(p)], axr.at[p])
            for to in column:
                give(p, z, 1 - xl, azs, azr, to)
        else:
            once(f"az{p}", agb.at[pl.ds(0, 3), 0, rows_of(p)], azr.at[p])
            for d in (1, 2, 3):
                give(p, rem(z + d, 4), xl, axs, axr, beside)

    def finish(p):
        m, off = CUTS[p], OFFS[p]
        if GATHER[p] == "x":
            once(f"az{p}", agb.at[pl.ds(0, 3), :, rows_of(p)], azr.at[p])
        else:
            once(f"az{p}", agb.at[pl.ds(0, 3), 0, rows_of(p)], azr.at[p])
            once(f"ax{p}", agb.at[:, 0, rows_of(p)], axr.at[p])
        with scope(f"out{p}"):
            for zz in range(4):
                for xx in range(2):
                    for i, start in enumerate((off, HALF + off)):
                        o_np[start : start + m, (xx * 4 + zz) * OWN : (xx * 4 + zz + 1) * OWN] = agb[
                            zz, xx, 2 * off + i * m : 2 * off + (i + 1) * m, :
                        ]

    def forward(k):
        once(f"ogx{k}", part_of(2, k), ogx.at[k])
        og_pass[k].start()

    run = {
        "out": out_unit, "fwd": forward, "unit": unit, "adam": adam, "rz": reduce_z, "outer": outer,
        "pass": pass_on, "inner": sum_inner, "end": finish,
    }
    for kind, *rest in TASKS:
        run[kind](*rest)

    with scope("drain"):
        await_bytes(ogg.at[pl.ds(0, 3 * TOK)], ogs)
        kept = pl.ds(0, 2 * OFFS[OUT])
        await_bytes(hs.at[:, :, kept], hss)
        await_bytes(ysend.at[:, kept], yss)
        await_bytes(hse, hes)
        await_bytes(yse, yes)
        await_bytes(xse, xes)
        await_bytes(rsz, rzs)
        for p in range(PIPES):
            await_bytes((xsend if SUM[p] == "z" else xrb).at[rows_of(p)], rxs)
            if SUM[p] == "d":
                await_bytes(ipx.at[rows_of(p)], ixs)
        for p in range(PIPES):
            x_first = GATHER[p] == "x"
            await_bytes(agb.at[0, 0, rows_of(p)] if x_first else agb.at[:, 0, rows_of(p)], axs)
            await_bytes(agb.at[pl.ds(0, 3), :, rows_of(p)] if x_first else agb.at[pl.ds(0, 3), 0, rows_of(p)], azs)
        await_bytes(ipr, ips_)


SLABS = 14


def write_out(params, momentum, one, two, o_params, o_momentum, o_one, o_two, wide, sem):
    copies = [
        pltpu.make_async_copy(a, b, sem.at[i])
        for i, (a, b) in enumerate(((one, o_one), (two, o_two), (momentum, o_momentum)))
    ]
    for q in copies:
        q.start()
    for k in range(SLABS):
        rows = pl.ds(k * (ROWS // SLABS), ROWS // SLABS)
        wide[rows, :] = params[rows, :].astype(F32)
        q = pltpu.make_async_copy(wide.at[rows], o_params.at[rows], sem.at[3 + k])
        q.start()
        copies.append(q)
    for q in copies:
        q.wait()


def per_device(hidden, out_grad, inner_params, first, second, outer_params, outer_momentum):
    any_ = pl.BlockSpec(memory_space=pl.ANY)
    dma, vmem = pltpu.SemaphoreType.DMA, pltpu.VMEM
    params, momentum, one, two = pl.pallas_call(
        kernel,
        out_shape=(
            vmem((ROWS, COLS), BF16),
            vmem((ROWS, OWN), F32),
            vmem((ROWS, COLS), BF16),
            vmem((ROWS, COLS), BF16),
        ),
        in_specs=[any_] * 7,
        out_specs=(pl.BlockSpec(memory_space=vmem),) * 4,
        scratch_shapes=[
            vmem((8, TOK, 2 * ROWS), BF16),
            vmem((3, YS, ROWS, TOK), BF16),
            vmem((YS, ROWS, 4 * TOK), BF16),
            vmem((4 * TOK, COLS), BF16),
            vmem((ROWS, COLS), F32),
            vmem((3, ROWS, COLS), BF16),
            vmem((3, ROWS, COLS), BF16),
            vmem((ROWS, COLS), F32),
            vmem((ROWS, COLS), BF16),
            vmem((ROWS, COLS), BF16),
            vmem((ROWS, OWN), F32),
            vmem((ROWS, OWN), F32),
            vmem((4, 2, ROWS, OWN), BF16),
            vmem((3, 2, ROWS, OWN), BF16),
            vmem((ROWS, OWN), F32),
            vmem((ROWS, OWN), F32),
            vmem((ROWS, OWN), F32),
            vmem((4, 2, ROWS, OWN), BF16),
            vmem((3, 2, ROWS, OWN), F32),
            vmem((ROWS, OWN), F32),
            vmem((ROWS, OWN), F32),
            vmem((ROWS, OWN), F32),
            vmem((ROWS, OWN), BF16),
            vmem((YS, 4 * CUTS[OUT], TOK), BF16),
            vmem((YS, 4 * CUTS[OUT], 2 * TOK), BF16),
            vmem((4 * CUTS[OUT], COLS), F32),
            vmem((3, 4 * CUTS[OUT], COLS), BF16),
            vmem((3, 4 * CUTS[OUT], COLS), BF16),
            vmem((2 * CUTS[OUT], COLS), BF16),
            vmem((2 * CUTS[OUT], COLS), BF16),
            dma((6,)),
            dma((8,)),
            dma,
            dma,
            dma((PARTS,)),
            dma((PARTS,)),
            dma,
            dma((YS,)),
            dma,
            dma((3,)),
            dma,
            dma,
            dma,
            dma((PIPES, YS)),
            dma,
            dma((PIPES, 3)),
            dma((PIPES, PARTS)),
            dma,
            dma((PIPES,)),
            dma,
            dma((PIPES,)),
            dma,
            dma((PIPES,)),
            dma,
            dma((PIPES,)),
            dma,
            dma,
            dma,
            dma((PIPES,)),
        ],
        compiler_params=pltpu.CompilerParams(
            collective_id=1, has_side_effects=True, vmem_limit_bytes=55_000_000
        ),
        name="step",
    )(hidden, out_grad, inner_params, first, second, outer_params, outer_momentum)
    params, momentum, one, two = pl.pallas_call(
        write_out,
        out_shape=(
            jax.ShapeDtypeStruct((ROWS, COLS), F32),
            jax.ShapeDtypeStruct((ROWS, OWN), F32),
            jax.ShapeDtypeStruct((ROWS, COLS), BF16),
            jax.ShapeDtypeStruct((ROWS, COLS), BF16),
        ),
        in_specs=[pl.BlockSpec(memory_space=vmem)] * 4,
        out_specs=(any_,) * 4,
        scratch_shapes=[vmem((ROWS, COLS), F32), dma((3 + SLABS,))],
        compiler_params=pltpu.CompilerParams(vmem_limit_bytes=8_000_000),
        name="write",
    )(params, momentum, one, two)
    return params, momentum, one[None], two[None]


def solution(mesh):
    return jax.shard_map(
        per_device,
        mesh=mesh,
        in_specs=(
            P(("rep", "fsdp"), None),
            P(("rep", "fsdp"), None),
            P("rep", "fsdp", None),
            P("rep", "fsdp", None),
            P("rep", "fsdp", None),
            P("fsdp", "rep"),
            P("fsdp", "rep"),
        ),
        out_specs=(
            P("fsdp", None),
            P("fsdp", "rep"),
            P("rep", "fsdp", None),
            P("rep", "fsdp", None),
        ),
        check_vma=False,
    )
```
